32 devices in a mesh: seq: 8 (over z, x), kvh: 4 (over y, core).
Axes of the slice: x: 2, y: 2, z: 4, core: 2. Of those that a mesh axis runs over, the one named last changes fastest.
Arguments:
- queries: bfloat16 [1024, 28, 128], P('seq', 'kvh'), may hold values from -80 to 80
- new_keys: bfloat16 [1024, 4, 128], P('seq', 'kvh'), may hold values from -8 to 8
- cache_keys: bfloat16 [512, 4, 128], P('seq', 'kvh'), may hold values from -1.1953125 to 1.1953125
- window_start: int32 [8], replicated, may hold values from 0 to 512, as said below
- owner_slot: int32 [8], replicated, may hold values from 0 to 511, as said below
Outputs:
- relevance: bfloat16 [1024, 28, 512], P('seq', 'kvh')
- rep_bank: bfloat16 [512, 4, 128], P('seq', 'kvh')
The draws below stay inside these ranges and needn't reach their ends.
Inputs may be any that keep to these rules, and one draw needn't show every extreme that they name: `window_start`: each window lies inside the new tokens; some window begins at the first new token and some ends at the last. `owner_slot`: the slots are distinct; the first and the last memory block are always among them.
All inputs are finite; a program needn't handle non-finite values.
Results may differ from the reference program's by a relative error of at most 0.0018.
Values may be sent and summed in bfloat16 or wider, within the bound.
A program may use at most 64 MiB of HBM per device.

```python
import math
import jax
import jax.numpy as jnp
from jax import lax

HEADS = 28
KVH = 4
HD = 128
BLK = 128
WIN = 512
QTOK = 1024
NEWB = 8
CACHEB = 512


def joint_draw(key):
    key_query = jax.random.fold_in(key, 11)
    key_keys = jax.random.fold_in(key, 12)
    key_window = jax.random.fold_in(key, 13)
    key_ends = jax.random.fold_in(key, 16)
    starts = jax.random.randint(key_window, (NEWB,), 0, QTOK - WIN + 1).astype(jnp.int32)
    end_keys = jax.random.split(key_ends, 2)
    first_pick = jax.random.randint(end_keys[0], (), 0, NEWB).astype(jnp.int32)
    second_pick = ((first_pick + 1 + jax.random.randint(end_keys[1], (), 0, NEWB - 1)) % NEWB).astype(jnp.int32)
    starts = starts.at[first_pick].set(jnp.int32(0))
    starts = starts.at[second_pick].set(jnp.int32(QTOK - WIN))
    key_rows = jnp.clip(jax.random.normal(key_keys, (QTOK, KVH, HD), jnp.float32), -8.0, 8.0)
    query_rows = jnp.clip(jax.random.normal(key_query, (QTOK, HEADS, HD), jnp.float32), -8.0, 8.0)
    return (query_rows, key_rows, starts)


def draw_queries(key, part):
    return joint_draw(key)[0].astype(jnp.bfloat16)


def draw_new_keys(key, part):
    return joint_draw(key)[1].astype(jnp.bfloat16)


def draw_window_start(key, part):
    return joint_draw(key)[2]


def draw_owner_slot(key, part):
    inner = jax.random.permutation(jax.random.fold_in(key, 21), CACHEB - 2)[:NEWB - 2].astype(jnp.int32) + 1
    ends = jnp.array([0, CACHEB - 1], dtype=jnp.int32)
    slots = jnp.concatenate([ends, inner])
    order = jax.random.permutation(jax.random.fold_in(key, 22), NEWB)
    return slots[order].astype(jnp.int32)


def block_scale(key, extent, cuts, low, largest):
    level, own = 1.0, jax.random.fold_in(key, 6)
    for position, shards_of in cuts:
        draws = jnp.exp(jax.random.uniform(jax.random.fold_in(own, position), (shards_of,), jnp.float32, low / len(cuts), largest / len(cuts)))
        level = level * jnp.repeat(draws, extent[position] // shards_of).reshape([-1 if axis == position else 1 for axis in range(len(extent))])
    return level


def normal_values(rng, shape, deviation, reach, pieces=(), held_as=jnp.bfloat16):
    level = block_scale(rng, shape, pieces, -0.22, 0.18) if pieces else 1.0
    values = jax.random.normal(rng, shape, jnp.float32) * deviation * level
    return jnp.minimum(jnp.maximum(values, -reach), reach).astype(held_as)


def setup_inputs(seed: int = 0) -> dict:
    key_list = jax.random.split(jax.random.key(seed), 6)
    queries = draw_queries(jax.random.fold_in(key_list[5], 71), 0)
    new_keys = draw_new_keys(jax.random.fold_in(key_list[5], 71), 0)
    cache_keys = normal_values(key_list[2], (CACHEB, KVH, HD), 0.15, 1.1953125, ((0, 8), (1, 4)))
    window_start = draw_window_start(jax.random.fold_in(key_list[5], 71), 0)
    owner_slot = draw_owner_slot(jax.random.fold_in(key_list[5], 71), 0)
    return {"queries": queries, "new_keys": new_keys, "cache_keys": cache_keys, "window_start": window_start, "owner_slot": owner_slot}


def reference(queries, new_keys, cache_keys, window_start, owner_slot):
    group_size = HEADS // KVH
    score_scale = 1.0 / math.sqrt(HD)

    def one_block(block_index):
        begin = window_start[block_index].astype(jnp.int32)
        window_q = lax.dynamic_slice_in_dim(queries, begin, WIN, 0).astype(jnp.float32)
        window_q = window_q.reshape(WIN, KVH, group_size, HD)
        block_keys = lax.dynamic_slice_in_dim(new_keys, (block_index * BLK).astype(jnp.int32), BLK, 0).astype(jnp.float32)
        scores = jnp.einsum('wgjd,kgd->wgjk', window_q, block_keys, precision=lax.Precision.HIGHEST) * score_scale
        softmax_weights = jax.nn.softmax(scores, axis=-1)
        weights = lax.optimization_barrier(jnp.sum(softmax_weights, axis=(0, 2))) / (group_size * WIN)
        merged = jnp.einsum('gk,kgd->gd', weights, block_keys, precision=lax.Precision.HIGHEST)
        return merged.astype(jnp.bfloat16)
    representative = lax.map(one_block, jnp.arange(NEWB, dtype=jnp.int32))
    key_bank = cache_keys.at[owner_slot].set(representative)
    query_block = math.gcd(QTOK, 512)
    bank_float = key_bank.astype(jnp.float32)

    def score_block(query_part):
        grouped = query_part.astype(jnp.float32).reshape(query_block, KVH, group_size, HD)
        result = jnp.einsum('tgjd,bgd->tgjb', grouped, bank_float) * score_scale
        return result.astype(jnp.bfloat16).reshape(query_block, HEADS, CACHEB)
    relevance = lax.map(score_block, queries.reshape(QTOK // query_block, query_block, HEADS, HD))
    return (relevance.reshape(QTOK, HEADS, CACHEB), key_bank)
```

```python
import functools
import math

import jax
import jax.numpy as jnp
from jax import lax
from jax.experimental import pallas as pl
from jax.experimental.pallas import tpu as pltpu
from jax.sharding import PartitionSpec as P

BLK = 128
WIN = 512
VMEM = 67043328
LOG2E = 1.4426950408889634
NT = (((1,), (1,)), ((), ()))


def each(count, body):
    if count <= 8:
        for i in range(count):
            body(i)
    else:
        lax.fori_loop(0, count, lambda i, c: (body(i), c)[1], 0)


def refresh_kernel(
    n, start_hbm, slot_hbm, q_hbm, k_hbm, c_hbm, q_v, bank,
    start_ref, slot_ref, q_t, keys, cache, mine, parts,
    load_sem, ks_sem, kr_sem, cs_sem, cr_sem, ps_sem, pr_sem,
):
    group, toks, dim = q_v.shape
    ktoks = keys.shape[1]
    local = cache.shape[1]
    slots = n * local
    per = ktoks // BLK
    blocks = n * per
    rows = group * toks
    scale = 1.0 / math.sqrt(dim)
    me = lax.axis_index("seq")

    load_k = pltpu.make_async_copy(k_hbm, keys.at[me], load_sem.at[0])
    load_q = pltpu.make_async_copy(q_hbm, q_v, load_sem.at[1])
    load_c = pltpu.make_async_copy(c_hbm, cache.at[me], load_sem.at[2])
    load_w = pltpu.make_async_copy(start_hbm, start_ref, load_sem.at[3])
    load_s = pltpu.make_async_copy(slot_hbm, slot_ref, load_sem.at[4])
    load_k.start()
    load_c.start()
    load_q.start()
    load_w.start()
    load_s.start()

    barrier = pltpu.get_barrier_semaphore()

    def greet(i):
        peer = lax.rem(me + 1 + i, n)
        pl.semaphore_signal(
            barrier, inc=1, device_id={"seq": peer}, device_id_type=pl.DeviceIdType.MESH
        )

    each(n - 1, greet)

    def link(src, dst, s_sem, r_sem, peer):
        return pltpu.make_async_remote_copy(
            src_ref=src, dst_ref=dst, send_sem=s_sem, recv_sem=r_sem,
            device_id={"seq": peer}, device_id_type=pl.DeviceIdType.MESH,
        )

    def key_copy(slot, peer):
        return link(keys.at[slot], keys.at[slot], ks_sem.at[peer], kr_sem.at[slot], peer)

    def cache_copy(slot, peer):
        return link(cache.at[slot], cache.at[slot], cs_sem.at[peer], cr_sem.at[slot], peer)

    def part_copy(slot, peer, src):
        return link(src, parts.at[slot], ps_sem.at[peer], pr_sem.at[slot], peer)

    load_q.wait()
    load_w.wait()
    load_s.wait()
    for j in range(group):
        q_t[:, j * toks:(j + 1) * toks] = q_v[j].T

    load_k.wait()
    position = me * toks + lax.broadcasted_iota(jnp.int32, (1, toks), 1)

    def partial(owner):
        for p in range(per):
            index = owner * per + p
            kb = keys[owner, p * BLK:(p + 1) * BLK, :]
            begin = start_ref[index]
            mask = jnp.where((position >= begin) & (position < begin + WIN), 1.0, 0.0)
            s = jnp.dot(kb, q_t[...], preferred_element_type=jnp.float32)
            top = jnp.max(s, axis=0, keepdims=True)
            e = jnp.exp2((s - top) * (scale * LOG2E))
            total = jnp.sum(e, axis=0, keepdims=True)
            acc = None
            for j in range(group):
                cols = slice(j * toks, (j + 1) * toks)
                term = e[:, cols] * (mask / total[:, cols])
                acc = term if acc is None else acc + term
            weight = jnp.sum(acc, axis=1, keepdims=True)
            rep = jnp.sum(weight * kb.astype(jnp.float32), axis=0, keepdims=True)
            mine[pl.ds(index, 1), :] = rep

    partial(me)

    pl.semaphore_wait(barrier, n - 1)
    each(n - 1, lambda i: key_copy(me, lax.rem(me + 1 + i, n)).start())
    load_c.wait()

    def arrive(i):
        owner = lax.rem(me + n - 1 - i, n)
        key_copy(owner, owner).wait_recv()
        partial(owner)

    each(n - 1, arrive)
    each(n - 1, lambda i: part_copy(me, lax.rem(me + 1 + i, n), mine).start())
    each(n - 1, lambda i: cache_copy(me, lax.rem(me + 1 + i, n)).start())

    each(n - 1, lambda i: cache_copy(lax.rem(me + n - 1 - i, n), me).wait_recv())
    hits = jnp.where(
        lax.broadcasted_iota(jnp.int32, (slots, blocks), 0) == slot_ref[...], 1.0, 0.0
    )
    taken = jnp.max(hits, axis=1, keepdims=True)
    hits = hits.astype(jnp.bfloat16)
    old = cache[...].reshape(slots, dim)

    each(n - 1, lambda i: part_copy(lax.rem(me + n - 1 - i, n), me, mine).wait_recv())
    parts[me] = mine[...]
    if n <= 8:
        rep_sum = parts[0]
        for d in range(1, n):
            rep_sum = rep_sum + parts[d]
    else:
        rep_sum = lax.fori_loop(1, n, lambda d, c: c + parts[d], parts[0])
    rep = (rep_sum * (1.0 / (group * WIN))).astype(jnp.bfloat16)
    placed = jnp.dot(hits, rep, preferred_element_type=jnp.float32)
    bank[...] = jnp.where(taken > 0.5, placed, old.astype(jnp.float32)).astype(jnp.bfloat16)
    def drain(i):
        peer = lax.rem(me + 1 + i, n)
        key_copy(me, peer).wait_send()
        cache_copy(me, peer).wait_send()
        part_copy(me, peer, mine).wait_send()

    each(n - 1, drain)


def line_kernel(
    n, start_hbm, slot_hbm, q_hbm, k_hbm, c_hbm, q_v, bank,
    start_ref, slot_ref, q_t, keys, cache, mine, parts,
    load_sem, ready, ks_sem, kf_sem, kr_sem, cs_sem, cf_sem, cr_sem, ps_sem, pr_sem,
):
    group, toks, dim = q_v.shape
    ktoks = keys.shape[1]
    local = cache.shape[1]
    slots = n * local
    per = ktoks // BLK
    blocks = n * per
    rows = n // 2
    scale = 1.0 / math.sqrt(dim)
    me = lax.axis_index("seq")
    row = me // 2
    side = me % 2
    pair = me + 1 - 2 * side

    load_k = pltpu.make_async_copy(k_hbm, keys.at[me], load_sem.at[0])
    load_q = pltpu.make_async_copy(q_hbm, q_v, load_sem.at[1])
    load_c = pltpu.make_async_copy(c_hbm, cache.at[me], load_sem.at[2])
    load_w = pltpu.make_async_copy(start_hbm, start_ref, load_sem.at[3])
    load_s = pltpu.make_async_copy(slot_hbm, slot_ref, load_sem.at[4])
    load_k.start()
    load_q.start()
    load_c.start()
    load_w.start()
    load_s.start()

    barrier = pltpu.get_barrier_semaphore()

    def signal(sem, peer):
        pl.semaphore_signal(
            sem, inc=1, device_id={"seq": peer}, device_id_type=pl.DeviceIdType.MESH
        )

    def mate(other):
        return 2 * other + side

    @pl.when(side == 0)
    def _():
        signal(barrier, pair)

    for other in range(1, rows):
        @pl.when(other > row)
        def _(other=other):
            signal(barrier, mate(other))

        @pl.when((other > row) & (side == 0))
        def _(other=other):
            signal(barrier, mate(other) + 1)

    @pl.when(me > 0)
    def _():
        pl.semaphore_wait(barrier, row + side * (row + 1))

    @pl.when(side == 1)
    def _():
        signal(ready.at[me], pair)

    for other in reversed(range(rows - 1)):
        @pl.when(other < row)
        def _(other=other):
            signal(ready.at[me], mate(other))

        @pl.when((other < row) & (side == 1))
        def _(other=other):
            signal(ready.at[me], mate(other) - 1)

    def link(src, dst, s_sem, r_sem, peer):
        return pltpu.make_async_remote_copy(
            src_ref=src, dst_ref=dst, send_sem=s_sem, recv_sem=r_sem,
            device_id={"seq": peer}, device_id_type=pl.DeviceIdType.MESH,
        )

    def key_copy(slot, peer, sem):
        return link(keys.at[slot], keys.at[slot], sem, kr_sem.at[slot], peer)

    def cache_copy(slot, peer, sem):
        return link(cache.at[slot], cache.at[slot], sem, cr_sem.at[slot], peer)

    def part_copy(slot, peer, src):
        return link(src, parts.at[slot], ps_sem.at[peer], pr_sem.at[slot], peer)

    def own_key(peer):
        return key_copy(me, peer, ks_sem.at[peer])

    def own_cache(peer):
        return cache_copy(me, peer, cs_sem.at[peer])

    def partial(owner):
        for p in range(per):
            index = owner * per + p
            kb = keys[owner, p * BLK:(p + 1) * BLK, :]
            begin = start_ref[index]
            mask = jnp.where((position >= begin) & (position < begin + WIN), 1.0, 0.0)
            s = jnp.dot(kb, q_t[...], preferred_element_type=jnp.float32)
            top = jnp.max(s, axis=0, keepdims=True)
            e = jnp.exp2((s - top) * (scale * LOG2E))
            total = jnp.sum(e, axis=0, keepdims=True)
            acc = None
            for j in range(group):
                cols = slice(j * toks, (j + 1) * toks)
                term = e[:, cols] * (mask / total[:, cols])
                acc = term if acc is None else acc + term
            weight = jnp.sum(acc, axis=1, keepdims=True)
            rep = jnp.sum(weight * kb.astype(jnp.float32), axis=0, keepdims=True)
            mine[pl.ds(index, 1), :] = rep

    load_k.wait()

    @pl.when(side == 1)
    def _():
        own_key(pair).start()

    for dist in range(1, rows):
        @pl.when(row - dist >= 0)
        def _(dist=dist):
            own_key(me - 2 * dist).start()

        if dist in ():
            @pl.when((row - dist >= 0) & (side == 1))
            def _(dist=dist):
                own_key(me - 2 * dist - 1).start()

    def later(dist):
        @pl.when(row + dist < rows)
        def _():
            peer = me + 2 * dist
            pl.semaphore_wait(ready.at[peer], 1)
            own_key(peer).start()

        @pl.when((row + dist < rows) & (side == 0))
        def _():
            pl.semaphore_wait(ready.at[me + 2 * dist + 1], 1)

        if dist in ():
            @pl.when(row + dist < rows)
            def _():
                own_key(me + 2 * dist + 1 - 2 * side).start()

    @pl.when(side == 0)
    def _():
        pl.semaphore_wait(ready.at[pair], 1)
        own_key(pair).start()

    for dist in ():
        @pl.when((row - dist >= 0) & (side == 0))
        def _(dist=dist):
            own_key(me - 2 * dist + 1).start()

    later(1)

    load_q.wait()
    load_w.wait()
    load_s.wait()
    for j in range(group):
        q_t[:, j * toks:(j + 1) * toks] = q_v[j].T
    position = me * toks + lax.broadcasted_iota(jnp.int32, (1, toks), 1)
    later(2)
    partial(me)
    for dist in range(3, rows):
        later(dist)

    def pick(values):
        out = values[0]
        for r in range(1, rows):
            if values[r] != values[0]:
                out = jnp.where(row == r, values[r], out)
        return out

    near = [sorted((r for r in range(rows) if r != z), key=lambda r: (abs(r - z), r)) for z in range(rows)]
    def due(z, other, cross):
        dist = abs(z - other)
        when = 5.0 + 0.5 * dist
        if cross and dist not in ():
            return when + 3.6
        return when + (1.0 if cross else 0)

    order = [
        sorted((due(z, r, c), r, c, int(c == 0 and abs(r - z) not in ())) for r in near[z] for c in (0, 1))
        for z in range(rows)
    ]

    def fwd_key(owner):
        return key_copy(owner, pair, kf_sem.at[owner])

    def fwd_cache(owner):
        return cache_copy(owner, pair, cf_sem.at[owner])

    def chosen(step):
        z, cross, fwd = (pick([order[r][step][i] for r in range(rows)]) for i in (1, 2, 3))
        return 2 * z + side + cross * (1 - 2 * side), fwd

    def own_caches(act):
        act(own_cache(pair))
        for dist in range(1, rows):
            for peer, there in ((me + 2 * dist, row + dist < rows), (me - 2 * dist, row - dist >= 0)):
                @pl.when(there)
                def _(peer=peer):
                    act(own_cache(peer))

    key_copy(pair, pair, ks_sem.at[pair]).wait_recv()
    partial(pair)
    for step in range(len(order[0])):
        owner, fwd = chosen(step)
        key_copy(owner, owner, ks_sem.at[owner]).wait_recv()
        if isinstance(fwd, int):
            if fwd:
                fwd_key(owner).start()
        else:
            @pl.when(fwd == 1)
            def _(owner=owner):
                fwd_key(owner).start()
        if step == 2:
            load_c.wait()
            own_caches(lambda copy: copy.start())
        partial(owner)

    each(n - 1, lambda i: part_copy(me, lax.rem(me + 1 + i, n), mine).start())

    lines = [pick([near[z][i] for z in range(rows)]) for i in range(rows - 1)]
    for z in lines:
        owner = 2 * z + side
        cache_copy(owner, owner, cs_sem.at[owner]).wait_recv()
        fwd_cache(owner).start()
    cache_copy(pair, pair, cs_sem.at[pair]).wait_recv()
    for z in lines:
        owner = 2 * z + 1 - side
        cache_copy(owner, owner, cs_sem.at[owner]).wait_recv()
    hits = jnp.where(
        lax.broadcasted_iota(jnp.int32, (slots, blocks), 0) == slot_ref[...], 1.0, 0.0
    )
    taken = jnp.max(hits, axis=1, keepdims=True)
    hits = hits.astype(jnp.bfloat16)
    old = cache[...].reshape(slots, dim)

    each(n - 1, lambda i: part_copy(lax.rem(me + n - 1 - i, n), me, mine).wait_recv())
    parts[me] = mine[...]
    rep_sum = parts[0]
    for d in range(1, n):
        rep_sum = rep_sum + parts[d]
    rep = (rep_sum * (1.0 / (group * WIN))).astype(jnp.bfloat16)
    placed = jnp.dot(hits, rep, preferred_element_type=jnp.float32)
    bank[...] = jnp.where(taken > 0.5, placed, old.astype(jnp.float32)).astype(jnp.bfloat16)

    own_caches(lambda copy: copy.wait_send())
    own_key(pair).wait_send()
    for z in lines:
        owner = 2 * z + side
        own_key(owner).wait_send()
        fwd_cache(owner).wait_send()
    for dist in range(1, rows):
        for peer, there in ((me + 2 * dist, row + dist < rows), (me - 2 * dist, row - dist >= 0)):
            @pl.when(there)
            def _(peer=peer, dist=dist):
                if dist in ():
                    own_key(peer + 1 - 2 * side).wait_send()
                else:
                    fwd_key(peer).wait_send()
    each(n - 1, lambda i: part_copy(me, lax.rem(me + 1 + i, n), mine).wait_send())


def relate_kernel(q_v, bank, rel_hbm, bank_hbm, rel_v, sem):
    group, toks, dim = q_v.shape
    local = bank_hbm.shape[0]
    scale = 1.0 / math.sqrt(dim)
    first = pl.multiple_of(lax.axis_index("seq") * local, local)
    keep = pltpu.make_async_copy(bank.at[pl.ds(first, local)], bank_hbm, sem.at[group])
    keep.start()
    outs = [
        pltpu.make_async_copy(rel_v.at[j], rel_hbm.at[j], sem.at[j]) for j in range(group)
    ]
    for j in range(group):
        r = lax.dot_general(q_v[j], bank[...], NT, preferred_element_type=jnp.float32)
        rel_v[j] = (r * scale).astype(jnp.bfloat16)
        outs[j].start()
    for out in outs:
        out.wait()
    keep.wait()


def per_device(n, queries, new_keys, cache_keys, window_start, owner_slot):
    toks, group, dim = queries.shape
    ktoks, local = new_keys.shape[0], cache_keys.shape[0]
    blocks = window_start.shape[0]
    slots = n * local
    hbm_spec = pl.BlockSpec(memory_space=pltpu.HBM)
    vmem_spec = pl.BlockSpec(memory_space=pltpu.VMEM)
    bf16 = jnp.bfloat16
    short = n % 2 == 0 and n <= 8
    sems = [pltpu.SemaphoreType.DMA((n,))] * (8 if short else 6)
    if short:
        sems = [pltpu.SemaphoreType.REGULAR((n,))] + sems
    q_held, bank = pl.pallas_call(
        functools.partial(line_kernel if short else refresh_kernel, n),
        out_shape=(
            pltpu.VMEM((group, toks, dim), bf16),
            pltpu.VMEM((slots, dim), bf16),
        ),
        in_specs=[hbm_spec] * 5,
        out_specs=(vmem_spec, vmem_spec),
        scratch_shapes=[
            pltpu.SMEM((blocks,), jnp.int32),
            pltpu.VMEM((1, blocks), jnp.int32),
            pltpu.VMEM((dim, group * toks), bf16),
            pltpu.VMEM((n, ktoks, dim), bf16),
            pltpu.VMEM((n, local, dim), bf16),
            pltpu.VMEM((blocks, dim), jnp.float32),
            pltpu.VMEM((n, blocks, dim), jnp.float32),
            pltpu.SemaphoreType.DMA((5,)),
        ] + sems,
        compiler_params=pltpu.CompilerParams(
            collective_id=0, has_side_effects=True, vmem_limit_bytes=VMEM - 2 * dim * (group * toks + slots) - 16384
        ),
        name="refresh",
    )(
        window_start,
        owner_slot.reshape(1, blocks),
        jnp.transpose(queries, (1, 0, 2)),
        new_keys.reshape(ktoks, dim),
        cache_keys.reshape(local, dim),
    )
    rel, own = pl.pallas_call(
        relate_kernel,
        out_shape=(
            jax.ShapeDtypeStruct((group, toks, slots), bf16),
            jax.ShapeDtypeStruct((local, dim), bf16),
        ),
        in_specs=[vmem_spec, vmem_spec],
        out_specs=(hbm_spec, hbm_spec),
        scratch_shapes=[
            pltpu.VMEM((group, toks, slots), bf16),
            pltpu.SemaphoreType.DMA((group + 1,)),
        ],
        compiler_params=pltpu.CompilerParams(
            vmem_limit_bytes=2 * group * toks * slots + 16 * 1024 * 1024
        ),
        name="relate",
    )(q_held, bank)
    return jnp.transpose(rel, (1, 0, 2)), own[:, None, :]


def solution(mesh):
    spec = P("seq", "kvh", None)
    return jax.shard_map(
        functools.partial(per_device, mesh.shape["seq"]),
        mesh=mesh,
        in_specs=(spec, spec, spec, P(), P()),
        out_specs=(spec, spec),
        check_vma=False,
    )
```

```python
import functools
import math

import jax
import jax.numpy as jnp
from jax import lax
from jax.experimental import pallas as pl
from jax.experimental.pallas import tpu as pltpu
from jax.sharding import PartitionSpec as P

BLK = 128
WIN = 512
VMEM = 67043328
LOG2E = 1.4426950408889634
NT = (((1,), (1,)), ((), ()))


def each(count, body):
    if count <= 8:
        for i in range(count):
            body(i)
    else:
        lax.fori_loop(0, count, lambda i, c: (body(i), c)[1], 0)


def refresh_kernel(
    n, start_hbm, slot_hbm, q_hbm, k_hbm, c_hbm, q_v, bank,
    start_ref, slot_ref, q_t, keys, cache, mine, parts,
    load_sem, ks_sem, kr_sem, cs_sem, cr_sem, ps_sem, pr_sem,
):
    group, toks, dim = q_v.shape
    ktoks = keys.shape[1]
    local = cache.shape[1]
    slots = n * local
    per = ktoks // BLK
    blocks = n * per
    rows = group * toks
    scale = 1.0 / math.sqrt(dim)
    me = lax.axis_index("seq")

    load_k = pltpu.make_async_copy(k_hbm, keys.at[me], load_sem.at[0])
    load_q = pltpu.make_async_copy(q_hbm, q_v, load_sem.at[1])
    load_c = pltpu.make_async_copy(c_hbm, cache.at[me], load_sem.at[2])
    load_w = pltpu.make_async_copy(start_hbm, start_ref, load_sem.at[3])
    load_s = pltpu.make_async_copy(slot_hbm, slot_ref, load_sem.at[4])
    load_k.start()
    load_c.start()
    load_q.start()
    load_w.start()
    load_s.start()

    barrier = pltpu.get_barrier_semaphore()

    def greet(i):
        peer = lax.rem(me + 1 + i, n)
        pl.semaphore_signal(
            barrier, inc=1, device_id={"seq": peer}, device_id_type=pl.DeviceIdType.MESH
        )

    each(n - 1, greet)

    def link(src, dst, s_sem, r_sem, peer):
        return pltpu.make_async_remote_copy(
            src_ref=src, dst_ref=dst, send_sem=s_sem, recv_sem=r_sem,
            device_id={"seq": peer}, device_id_type=pl.DeviceIdType.MESH,
        )

    def key_copy(slot, peer):
        return link(keys.at[slot], keys.at[slot], ks_sem.at[peer], kr_sem.at[slot], peer)

    def cache_copy(slot, peer):
        return link(cache.at[slot], cache.at[slot], cs_sem.at[peer], cr_sem.at[slot], peer)

    def part_copy(slot, peer, src):
        return link(src, parts.at[slot], ps_sem.at[peer], pr_sem.at[slot], peer)

    load_q.wait()
    load_w.wait()
    load_s.wait()
    for j in range(group):
        q_t[:, j * toks:(j + 1) * toks] = q_v[j].T

    load_k.wait()
    position = me * toks + lax.broadcasted_iota(jnp.int32, (1, toks), 1)

    def partial(owner):
        for p in range(per):
            index = owner * per + p
            kb = keys[owner, p * BLK:(p + 1) * BLK, :]
            begin = start_ref[index]
            mask = jnp.where((position >= begin) & (position < begin + WIN), 1.0, 0.0)
            s = jnp.dot(kb, q_t[...], preferred_element_type=jnp.float32)
            top = jnp.max(s, axis=0, keepdims=True)
            e = jnp.exp2((s - top) * (scale * LOG2E))
            total = jnp.sum(e, axis=0, keepdims=True)
            acc = None
            for j in range(group):
                cols = slice(j * toks, (j + 1) * toks)
                term = e[:, cols] * (mask / total[:, cols])
                acc = term if acc is None else acc + term
            weight = jnp.sum(acc, axis=1, keepdims=True)
            rep = jnp.sum(weight * kb.astype(jnp.float32), axis=0, keepdims=True)
            mine[pl.ds(index, 1), :] = rep

    partial(me)

    pl.semaphore_wait(barrier, n - 1)
    each(n - 1, lambda i: key_copy(me, lax.rem(me + 1 + i, n)).start())
    load_c.wait()

    def arrive(i):
        owner = lax.rem(me + n - 1 - i, n)
        key_copy(owner, owner).wait_recv()
        partial(owner)

    each(n - 1, arrive)
    each(n - 1, lambda i: part_copy(me, lax.rem(me + 1 + i, n), mine).start())
    each(n - 1, lambda i: cache_copy(me, lax.rem(me + 1 + i, n)).start())

    each(n - 1, lambda i: cache_copy(lax.rem(me + n - 1 - i, n), me).wait_recv())
    hits = jnp.where(
        lax.broadcasted_iota(jnp.int32, (slots, blocks), 0) == slot_ref[...], 1.0, 0.0
    )
    taken = jnp.max(hits, axis=1, keepdims=True)
    hits = hits.astype(jnp.bfloat16)
    old = cache[...].reshape(slots, dim)

    each(n - 1, lambda i: part_copy(lax.rem(me + n - 1 - i, n), me, mine).wait_recv())
    parts[me] = mine[...]
    if n <= 8:
        rep_sum = parts[0]
        for d in range(1, n):
            rep_sum = rep_sum + parts[d]
    else:
        rep_sum = lax.fori_loop(1, n, lambda d, c: c + parts[d], parts[0])
    rep = (rep_sum * (1.0 / (group * WIN))).astype(jnp.bfloat16)
    placed = jnp.dot(hits, rep, preferred_element_type=jnp.float32)
    bank[...] = jnp.where(taken > 0.5, placed, old.astype(jnp.float32)).astype(jnp.bfloat16)
    def drain(i):
        peer = lax.rem(me + 1 + i, n)
        key_copy(me, peer).wait_send()
        cache_copy(me, peer).wait_send()
        part_copy(me, peer, mine).wait_send()

    each(n - 1, drain)


FAR = [3, 9]
CHAIN = [0, 0]
UP_AT = [1, 1]
DOWN_AT = [5, 5]
PAIR_AT = [3, 3]
HAND_UP = [4, 5, 6]
HAND_DOWN = [7, 7, 7]
T_PAIR = [5.0, 3.9]
T_LINE = [4.9, 4.0]
T_HOP = [0.9, 2.2]
T_RELAY = [3.2, 2.2]
T_FAR = [7.0, 9.0]


def plan(rows, group):
    far, chain = FAR[group], CHAIN[group]
    table = []
    for z in range(rows):
        blocks = [(T_PAIR[group], z, 1, 0, tuple(r for r in range(rows) if r - z >= far))]
        for r in range(rows):
            if r == z:
                continue
            line = T_LINE[group] + T_HOP[group] * (abs(r - z) - 1)
            on = z + (1 if z > r else -1)
            blocks.append((line, r, 0, int(z - r < far), (on,) if chain and 0 <= on < rows else ()))
            blocks.append((T_FAR[group] if z - r >= far else line + T_RELAY[group], r, 1, 0, ()))
        table.append([b[1:] for b in sorted(blocks)])
    return table


def line_kernel(
    n, start_hbm, slot_hbm, q_hbm, k_hbm, c_hbm, q_v, bank,
    start_ref, slot_ref, q_t, keys, cache, mine, parts,
    load_sem, ready, ks_sem, kf_sem, kl_sem, kr_sem, cs_sem, cf_sem, cr_sem, ps_sem, pr_sem,
):
    group, toks, dim = q_v.shape
    ktoks = keys.shape[1]
    local = cache.shape[1]
    slots = n * local
    per = ktoks // BLK
    blocks = n * per
    rows = n // 2
    scale = 1.0 / math.sqrt(dim)
    me = lax.axis_index("seq")
    second = lax.axis_index("kvh") % 2
    row = me // 2
    side = me % 2
    pair = me + 1 - 2 * side

    load_k = pltpu.make_async_copy(k_hbm, keys.at[me], load_sem.at[0])
    load_q = pltpu.make_async_copy(q_hbm, q_v, load_sem.at[1])
    load_c = pltpu.make_async_copy(c_hbm, cache.at[me], load_sem.at[2])
    load_w = pltpu.make_async_copy(start_hbm, start_ref, load_sem.at[3])
    load_s = pltpu.make_async_copy(slot_hbm, slot_ref, load_sem.at[4])
    load_k.start()
    load_q.start()
    load_c.start()
    load_w.start()
    load_s.start()

    barrier = pltpu.get_barrier_semaphore()

    def signal(sem, peer):
        pl.semaphore_signal(
            sem, inc=1, device_id={"seq": peer}, device_id_type=pl.DeviceIdType.MESH
        )

    def when(flag, act):
        if isinstance(flag, (bool, int)):
            if flag:
                act()
        else:
            pl.when(flag)(act)

    def mate(other):
        return 2 * other + side

    when(side == 0, lambda: signal(barrier, pair))
    for other in range(1, rows):
        when(other > row, lambda: signal(barrier, mate(other)))

    when(me > 0, lambda: pl.semaphore_wait(barrier, row + side))
    when(side == 1, lambda: signal(ready.at[me], pair))
    for other in reversed(range(rows - 1)):
        when(other < row, lambda: signal(ready.at[me], mate(other)))

    def link(src, dst, s_sem, r_sem, peer):
        return pltpu.make_async_remote_copy(
            src_ref=src, dst_ref=dst, send_sem=s_sem, recv_sem=r_sem,
            device_id={"seq": peer}, device_id_type=pl.DeviceIdType.MESH,
        )

    def key_copy(slot, peer, sem):
        return link(keys.at[slot], keys.at[slot], sem, kr_sem.at[slot], peer)

    def cache_copy(slot, peer, sem):
        return link(cache.at[slot], cache.at[slot], sem, cr_sem.at[slot], peer)

    def part_copy(slot, peer, src):
        return link(src, parts.at[slot], ps_sem.at[peer], pr_sem.at[slot], peer)

    def own_key(peer):
        return key_copy(me, peer, ks_sem.at[peer])

    def own_cache(peer):
        return cache_copy(me, peer, cs_sem.at[peer])

    def hand_key(owner):
        return key_copy(owner, pair, kf_sem.at[owner])

    def pass_key(owner, other):
        return key_copy(owner, mate(other), kl_sem.at[owner * rows + other])

    def hand_cache(owner):
        return cache_copy(owner, pair, cf_sem.at[owner])

    def pick(values):
        flat = [v for group in values for v in group]
        if len(set(flat)) == 1:
            return flat[0]
        out = flat[0]
        for at, v in enumerate(flat):
            if v != flat[0]:
                out = jnp.where(second * rows + row == at, v, out)
        return out

    tables = [plan(rows, g) for g in range(2)]

    def block(step):
        z, cross, to_pair = (
            pick([[t[r][step][i] for r in range(rows)] for t in tables]) for i in range(3)
        )
        onward = [
            (other, pick([[int(other in t[r][step][3]) for r in range(rows)] for t in tables]))
            for other in range(rows)
        ]
        return mate(z) + cross * (1 - 2 * side), to_pair, onward

    def flag(value):
        return bool(value) if isinstance(value, int) else value == 1

    def relays(step, act):
        owner, to_pair, onward = block(step)
        when(flag(to_pair), lambda: act(hand_key(owner)))
        for other, there in onward:
            when(flag(there), lambda: act(pass_key(owner, other)))

    def line_key(dist, act):
        there = (0 <= row + dist) & (row + dist < rows)
        straight = [abs(dist) == 1 or not chain for chain in CHAIN]
        if not all(straight):
            there = there & (second == straight.index(True)) if any(straight) else False
        when(there, lambda: act(own_key(me + 2 * dist)))

    def up_caches(act):
        for dist in range(1, rows):
            when(row - dist >= 0, lambda: act(own_cache(me - 2 * dist)))

    def down_caches(act):
        for dist in range(1, rows):
            when(row + dist < rows, lambda: act(own_cache(me + 2 * dist)))

    def at_step(places, step, act):
        if all(p == step for p in places):
            act()
        else:
            for g, p in enumerate(places):
                if p == step:
                    when(second == g, act)

    lines = [
        pick([[sorted((abs(r - z), r) for r in range(rows) if r != z)[i][1] for z in range(rows)]] * 2)
        for i in range(rows - 1)
    ]

    def caches(step):
        at_step(UP_AT, step, lambda: up_caches(lambda copy: copy.start()))
        at_step(DOWN_AT, step, lambda: down_caches(lambda copy: copy.start()))
        at_step(PAIR_AT, step, lambda: own_cache(pair).start())

        def hand(peer):
            cache_copy(peer, peer, cs_sem.at[peer]).wait_recv()
            hand_cache(peer).start()

        for dist in range(1, rows):
            if HAND_UP[dist - 1] == step:
                when(row + dist < rows, lambda: hand(me + 2 * dist))
            if HAND_DOWN[dist - 1] == step:
                when(row - dist >= 0, lambda: hand(me - 2 * dist))

    def partial(owner):
        for p in range(per):
            index = owner * per + p
            kb = keys[owner, p * BLK:(p + 1) * BLK, :]
            begin = start_ref[index]
            mask = jnp.where((position >= begin) & (position < begin + WIN), 1.0, 0.0)
            s = jnp.dot(kb, q_t[...], preferred_element_type=jnp.float32)
            top = jnp.max(s, axis=0, keepdims=True)
            e = jnp.exp2((s - top) * (scale * LOG2E))
            total = jnp.sum(e, axis=0, keepdims=True)
            acc = None
            for j in range(group):
                cols = slice(j * toks, (j + 1) * toks)
                term = e[:, cols] * (mask / total[:, cols])
                acc = term if acc is None else acc + term
            weight = jnp.sum(acc, axis=1, keepdims=True)
            rep = jnp.sum(weight * kb.astype(jnp.float32), axis=0, keepdims=True)
            mine[pl.ds(index, 1), :] = rep

    load_k.wait()

    when(side == 1, lambda: own_key(pair).start())
    for dist in range(1, rows):
        line_key(-dist, lambda copy: copy.start())

    def later(dist):
        when(row + dist < rows, lambda: pl.semaphore_wait(ready.at[me + 2 * dist], 1))
        line_key(dist, lambda copy: copy.start())

    def to_pair():
        pl.semaphore_wait(ready.at[pair], 1)
        own_key(pair).start()

    when(side == 0, to_pair)
    later(1)
    load_q.wait()
    load_w.wait()
    load_s.wait()
    for j in range(group):
        q_t[:, j * toks:(j + 1) * toks] = q_v[j].T
    position = me * toks + lax.broadcasted_iota(jnp.int32, (1, toks), 1)
    later(2)
    partial(me)
    for dist in range(3, rows):
        later(dist)
    load_c.wait()
    caches(-1)

    done = 0
    for step in range(n - 1):
        owner = block(step)[0]
        key_copy(owner, owner, ks_sem.at[owner]).wait_recv()
        relays(step, lambda copy: copy.start())
        caches(step)
        if step >= 2 - 1:
            for at in range(done, step + 1):
                partial(block(at)[0])
            done = step + 1

    each(n - 1, lambda i: part_copy(me, lax.rem(me + 1 + i, n), mine).start())
    caches(n - 1)
    cache_copy(pair, pair, cs_sem.at[pair]).wait_recv()
    for z in lines:
        owner = mate(z) + 1 - 2 * side
        cache_copy(owner, owner, cs_sem.at[owner]).wait_recv()
    hits = jnp.where(
        lax.broadcasted_iota(jnp.int32, (slots, blocks), 0) == slot_ref[...], 1.0, 0.0
    )
    taken = jnp.max(hits, axis=1, keepdims=True)
    hits = hits.astype(jnp.bfloat16)
    old = cache[...].reshape(slots, dim)

    each(n - 1, lambda i: part_copy(lax.rem(me + n - 1 - i, n), me, mine).wait_recv())
    parts[me] = mine[...]
    rep_sum = parts[0]
    for d in range(1, n):
        rep_sum = rep_sum + parts[d]
    rep = (rep_sum * (1.0 / (group * WIN))).astype(jnp.bfloat16)
    placed = jnp.dot(hits, rep, preferred_element_type=jnp.float32)
    bank[...] = jnp.where(taken > 0.5, placed, old.astype(jnp.float32)).astype(jnp.bfloat16)

    def sent(copy):
        copy.wait_send()

    sent(own_key(pair))
    sent(own_cache(pair))
    up_caches(sent)
    down_caches(sent)
    for dist in range(1, rows):
        line_key(-dist, sent)
        line_key(dist, sent)
    for z in lines:
        sent(hand_cache(mate(z)))
    for step in range(n - 1):
        relays(step, sent)
    each(n - 1, lambda i: sent(part_copy(me, lax.rem(me + 1 + i, n), mine)))


def relate_kernel(q_v, bank, rel_hbm, bank_hbm, rel_v, sem):
    group, toks, dim = q_v.shape
    local = bank_hbm.shape[0]
    scale = 1.0 / math.sqrt(dim)
    first = pl.multiple_of(lax.axis_index("seq") * local, local)
    keep = pltpu.make_async_copy(bank.at[pl.ds(first, local)], bank_hbm, sem.at[group])
    keep.start()
    outs = [
        pltpu.make_async_copy(rel_v.at[j], rel_hbm.at[j], sem.at[j]) for j in range(group)
    ]
    for j in range(group):
        r = lax.dot_general(q_v[j], bank[...], NT, preferred_element_type=jnp.float32)
        rel_v[j] = (r * scale).astype(jnp.bfloat16)
        outs[j].start()
    for out in outs:
        out.wait()
    keep.wait()


def per_device(n, queries, new_keys, cache_keys, window_start, owner_slot):
    toks, group, dim = queries.shape
    ktoks, local = new_keys.shape[0], cache_keys.shape[0]
    blocks = window_start.shape[0]
    slots = n * local
    hbm_spec = pl.BlockSpec(memory_space=pltpu.HBM)
    vmem_spec = pl.BlockSpec(memory_space=pltpu.VMEM)
    bf16 = jnp.bfloat16
    short = n % 2 == 0 and n <= 8
    sems = [pltpu.SemaphoreType.DMA((n,))] * 6
    if short:
        sems = (
            [pltpu.SemaphoreType.REGULAR((n,))]
            + [pltpu.SemaphoreType.DMA((n,))] * 2
            + [pltpu.SemaphoreType.DMA((n * n // 2,))]
            + [pltpu.SemaphoreType.DMA((n,))] * 6
        )
    q_held, bank = pl.pallas_call(
        functools.partial(line_kernel if short else refresh_kernel, n),
        out_shape=(
            pltpu.VMEM((group, toks, dim), bf16),
            pltpu.VMEM((slots, dim), bf16),
        ),
        in_specs=[hbm_spec] * 5,
        out_specs=(vmem_spec, vmem_spec),
        scratch_shapes=[
            pltpu.SMEM((blocks,), jnp.int32),
            pltpu.VMEM((1, blocks), jnp.int32),
            pltpu.VMEM((dim, group * toks), bf16),
            pltpu.VMEM((n, ktoks, dim), bf16),
            pltpu.VMEM((n, local, dim), bf16),
            pltpu.VMEM((blocks, dim), jnp.float32),
            pltpu.VMEM((n, blocks, dim), jnp.float32),
            pltpu.SemaphoreType.DMA((5,)),
        ] + sems,
        compiler_params=pltpu.CompilerParams(
            collective_id=0, has_side_effects=True, vmem_limit_bytes=VMEM - 2 * dim * (group * toks + slots) - 16384
        ),
        name="refresh",
    )(
        window_start,
        owner_slot.reshape(1, blocks),
        jnp.transpose(queries, (1, 0, 2)),
        new_keys.reshape(ktoks, dim),
        cache_keys.reshape(local, dim),
    )
    rel, own = pl.pallas_call(
        relate_kernel,
        out_shape=(
            jax.ShapeDtypeStruct((group, toks, slots), bf16),
            jax.ShapeDtypeStruct((local, dim), bf16),
        ),
        in_specs=[vmem_spec, vmem_spec],
        out_specs=(hbm_spec, hbm_spec),
        scratch_shapes=[
            pltpu.VMEM((group, toks, slots), bf16),
            pltpu.SemaphoreType.DMA((group + 1,)),
        ],
        compiler_params=pltpu.CompilerParams(
            vmem_limit_bytes=2 * group * toks * slots + 16 * 1024 * 1024
        ),
        name="relate",
    )(q_held, bank)
    return jnp.transpose(rel, (1, 0, 2)), own[:, None, :]


def solution(mesh):
    spec = P("seq", "kvh", None)
    return jax.shard_map(
        functools.partial(per_device, mesh.shape["seq"]),
        mesh=mesh,
        in_specs=(spec, spec, spec, P(), P()),
        out_specs=(spec, spec),
        check_vma=False,
    )
```

```python
import functools
import math

import jax
import jax.numpy as jnp
from jax import lax
from jax.experimental import pallas as pl
from jax.experimental.pallas import tpu as pltpu
from jax.sharding import PartitionSpec as P

BLK = 128
WIN = 512
VMEM = 67043328
LOG2E = 1.4426950408889634
NT = (((1,), (1,)), ((), ()))


def each(count, body):
    if count <= 8:
        for i in range(count):
            body(i)
    else:
        lax.fori_loop(0, count, lambda i, c: (body(i), c)[1], 0)


def refresh_kernel(
    n, start_hbm, slot_hbm, q_hbm, k_hbm, c_hbm, q_v, bank,
    start_ref, slot_ref, q_t, keys, cache, mine, parts,
    load_sem, ks_sem, kr_sem, cs_sem, cr_sem, ps_sem, pr_sem,
):
    group, toks, dim = q_v.shape
    ktoks = keys.shape[1]
    local = cache.shape[1]
    slots = n * local
    per = ktoks // BLK
    blocks = n * per
    rows = group * toks
    scale = 1.0 / math.sqrt(dim)
    me = lax.axis_index("seq")

    load_k = pltpu.make_async_copy(k_hbm, keys.at[me], load_sem.at[0])
    load_q = pltpu.make_async_copy(q_hbm, q_v, load_sem.at[1])
    load_c = pltpu.make_async_copy(c_hbm, cache.at[me], load_sem.at[2])
    load_w = pltpu.make_async_copy(start_hbm, start_ref, load_sem.at[3])
    load_s = pltpu.make_async_copy(slot_hbm, slot_ref, load_sem.at[4])
    load_k.start()
    load_c.start()
    load_q.start()
    load_w.start()
    load_s.start()

    barrier = pltpu.get_barrier_semaphore()

    def greet(i):
        peer = lax.rem(me + 1 + i, n)
        pl.semaphore_signal(
            barrier, inc=1, device_id={"seq": peer}, device_id_type=pl.DeviceIdType.MESH
        )

    each(n - 1, greet)

    def link(src, dst, s_sem, r_sem, peer):
        return pltpu.make_async_remote_copy(
            src_ref=src, dst_ref=dst, send_sem=s_sem, recv_sem=r_sem,
            device_id={"seq": peer}, device_id_type=pl.DeviceIdType.MESH,
        )

    def key_copy(slot, peer):
        return link(keys.at[slot], keys.at[slot], ks_sem.at[peer], kr_sem.at[slot], peer)

    def cache_copy(slot, peer):
        return link(cache.at[slot], cache.at[slot], cs_sem.at[peer], cr_sem.at[slot], peer)

    def part_copy(slot, peer, src):
        return link(src, parts.at[slot], ps_sem.at[peer], pr_sem.at[slot], peer)

    load_q.wait()
    load_w.wait()
    load_s.wait()
    for j in range(group):
        q_t[:, j * toks:(j + 1) * toks] = q_v[j].T

    load_k.wait()
    position = me * toks + lax.broadcasted_iota(jnp.int32, (1, toks), 1)

    def partial(owner):
        for p in range(per):
            index = owner * per + p
            kb = keys[owner, p * BLK:(p + 1) * BLK, :]
            begin = start_ref[index]
            mask = jnp.where((position >= begin) & (position < begin + WIN), 1.0, 0.0)
            s = jnp.dot(kb, q_t[...], preferred_element_type=jnp.float32)
            top = jnp.max(s, axis=0, keepdims=True)
            e = jnp.exp2((s - top) * (scale * LOG2E))
            total = jnp.sum(e, axis=0, keepdims=True)
            acc = None
            for j in range(group):
                cols = slice(j * toks, (j + 1) * toks)
                term = e[:, cols] * (mask / total[:, cols])
                acc = term if acc is None else acc + term
            weight = jnp.sum(acc, axis=1, keepdims=True)
            rep = jnp.sum(weight * kb.astype(jnp.float32), axis=0, keepdims=True)
            mine[pl.ds(index, 1), :] = rep

    partial(me)

    pl.semaphore_wait(barrier, n - 1)
    each(n - 1, lambda i: key_copy(me, lax.rem(me + 1 + i, n)).start())
    load_c.wait()

    def arrive(i):
        owner = lax.rem(me + n - 1 - i, n)
        key_copy(owner, owner).wait_recv()
        partial(owner)

    each(n - 1, arrive)
    each(n - 1, lambda i: part_copy(me, lax.rem(me + 1 + i, n), mine).start())
    each(n - 1, lambda i: cache_copy(me, lax.rem(me + 1 + i, n)).start())

    each(n - 1, lambda i: cache_copy(lax.rem(me + n - 1 - i, n), me).wait_recv())
    hits = jnp.where(
        lax.broadcasted_iota(jnp.int32, (slots, blocks), 0) == slot_ref[...], 1.0, 0.0
    )
    taken = jnp.max(hits, axis=1, keepdims=True)
    hits = hits.astype(jnp.bfloat16)
    old = cache[...].reshape(slots, dim)

    each(n - 1, lambda i: part_copy(lax.rem(me + n - 1 - i, n), me, mine).wait_recv())
    parts[me] = mine[...]
    if n <= 8:
        rep_sum = parts[0]
        for d in range(1, n):
            rep_sum = rep_sum + parts[d]
    else:
        rep_sum = lax.fori_loop(1, n, lambda d, c: c + parts[d], parts[0])
    rep = (rep_sum * (1.0 / (group * WIN))).astype(jnp.bfloat16)
    placed = jnp.dot(hits, rep, preferred_element_type=jnp.float32)
    bank[...] = jnp.where(taken > 0.5, placed, old.astype(jnp.float32)).astype(jnp.bfloat16)
    def drain(i):
        peer = lax.rem(me + 1 + i, n)
        key_copy(me, peer).wait_send()
        cache_copy(me, peer).wait_send()
        part_copy(me, peer, mine).wait_send()

    each(n - 1, drain)


FAR = [2, 9]
UP = [(3,), ()]
CUP = [(1, 2, 3), ()]
DOWN = [(), ()]
T_DIAG = [0.8, 0.8]
CHAIN = [0, 0]
UP_AT = [2, 2]
DOWN_AT = [4, 4]
PAIR_AT = [3, 3]
HAND_UP = [7, 7, 7]
HAND_DOWN = [7, 7, 7]
T_PAIR = [4.0, 3.9]
T_LINE = [4.9, 4.0]
T_HOP = [0.9, 2.2]
T_RELAY = [3.2, 2.2]
T_FAR = [7.0, 9.0]


def plan(rows, group):
    far, chain = FAR[group], CHAIN[group]
    table = []

    def swaps(a, b):
        return b - a >= far and (b == rows - 1 or not 1)

    for z in range(rows):
        blocks = [(T_PAIR[group], z, 1, 0, tuple(r for r in range(rows) if swaps(z, r)))]
        for r in range(rows):
            if r == z:
                continue
            line = T_LINE[group] + T_HOP[group] * (abs(r - z) - 1)
            on = z + (1 if z > r else -1)
            straight = abs(r - z) in (DOWN if r < z else UP)[group] and (r > z or z == rows - 1 or not 0)
            blocks.append((line, r, 0, int(not swaps(r, z) and not straight), (on,) if chain and 0 <= on < rows else ()))
            other = line + (T_DIAG if straight else T_RELAY)[group]
            blocks.append((T_FAR[group] if swaps(r, z) else other, r, 1, 0, ()))
        table.append([b[1:] for b in sorted(blocks)])
    return table


def line_kernel(
    n, start_hbm, slot_hbm, q_hbm, k_hbm, c_hbm, q_v, bank,
    start_ref, slot_ref, q_t, keys, cache, mine, parts,
    load_sem, ready, ks_sem, kf_sem, kl_sem, kr_sem, cs_sem, cf_sem, cr_sem, ps_sem, pr_sem,
):
    group, toks, dim = q_v.shape
    ktoks = keys.shape[1]
    local = cache.shape[1]
    slots = n * local
    per = ktoks // BLK
    blocks = n * per
    rows = n // 2
    scale = 1.0 / math.sqrt(dim)
    me = lax.axis_index("seq")
    second = lax.axis_index("kvh") % 2
    row = me // 2
    side = me % 2
    pair = me + 1 - 2 * side

    load_k = pltpu.make_async_copy(k_hbm, keys.at[me], load_sem.at[0])
    load_q = pltpu.make_async_copy(q_hbm, q_v, load_sem.at[1])
    load_c = pltpu.make_async_copy(c_hbm, cache.at[me], load_sem.at[2])
    load_w = pltpu.make_async_copy(start_hbm, start_ref, load_sem.at[3])
    load_s = pltpu.make_async_copy(slot_hbm, slot_ref, load_sem.at[4])
    load_k.start()
    load_q.start()
    load_c.start()
    load_w.start()
    load_s.start()

    barrier = pltpu.get_barrier_semaphore()

    def signal(sem, peer):
        pl.semaphore_signal(
            sem, inc=1, device_id={"seq": peer}, device_id_type=pl.DeviceIdType.MESH
        )

    def when(flag, act):
        if isinstance(flag, (bool, int)):
            if flag:
                act()
        else:
            pl.when(flag)(act)

    def mate(other):
        return 2 * other + side

    when(side == 0, lambda: signal(barrier, pair))
    for other in range(1, rows):
        when(other > row, lambda: signal(barrier, mate(other)))

    def diagonal(sets, dist, there, act):
        there = (0 <= row + dist) & (row + dist < rows) & there
        if 0 and sets is DOWN:
            there = there & ((row == rows - 1) if dist < 0 else (row + dist == rows - 1))
        has = [abs(dist) in g for g in sets]
        if any(has):
            when(there if all(has) else there & (second == has.index(True)), act)

    both = [set(a) | set(b) | set(c) for a, b, c in zip(UP, DOWN, CUP)]
    for dist in range(1, rows):
        diagonal(both, dist, side == 0, lambda: signal(barrier, me + 2 * dist + 1))

    count = row + side
    for g in range(2):
        for dist in sorted(both[g]):
            count = count + jnp.where((side == 1) & (row >= dist) & (second == g), 1, 0)

    when(me > 0, lambda: pl.semaphore_wait(barrier, count))
    when(side == 1, lambda: signal(ready.at[me], pair))
    for other in reversed(range(rows - 1)):
        when(other < row, lambda: signal(ready.at[me], mate(other)))
    for dist in reversed(range(1, rows)):
        diagonal(DOWN, -dist, side == 1, lambda: signal(ready.at[me], me - 2 * dist - 1))

    def link(src, dst, s_sem, r_sem, peer):
        return pltpu.make_async_remote_copy(
            src_ref=src, dst_ref=dst, send_sem=s_sem, recv_sem=r_sem,
            device_id={"seq": peer}, device_id_type=pl.DeviceIdType.MESH,
        )

    def key_copy(slot, peer, sem):
        return link(keys.at[slot], keys.at[slot], sem, kr_sem.at[slot], peer)

    def cache_copy(slot, peer, sem):
        return link(cache.at[slot], cache.at[slot], sem, cr_sem.at[slot], peer)

    def part_copy(slot, peer, src):
        return link(src, parts.at[slot], ps_sem.at[peer], pr_sem.at[slot], peer)

    def own_key(peer):
        return key_copy(me, peer, ks_sem.at[peer])

    def own_cache(peer):
        return cache_copy(me, peer, cs_sem.at[peer])

    def hand_key(owner):
        return key_copy(owner, pair, kf_sem.at[owner])

    def pass_key(owner, other):
        return key_copy(owner, mate(other), kl_sem.at[owner * rows + other])

    def hand_cache(owner):
        return cache_copy(owner, pair, cf_sem.at[owner])

    def pick(values):
        flat = [v for group in values for v in group]
        if len(set(flat)) == 1:
            return flat[0]
        out = flat[0]
        for at, v in enumerate(flat):
            if v != flat[0]:
                out = jnp.where(second * rows + row == at, v, out)
        return out

    tables = [plan(rows, g) for g in range(2)]

    def block(step):
        z, cross, to_pair = (
            pick([[t[r][step][i] for r in range(rows)] for t in tables]) for i in range(3)
        )
        onward = [
            (other, pick([[int(other in t[r][step][3]) for r in range(rows)] for t in tables]))
            for other in range(rows)
        ]
        return mate(z) + cross * (1 - 2 * side), to_pair, onward

    def flag(value):
        return bool(value) if isinstance(value, int) else value == 1

    def relays(step, act):
        owner, to_pair, onward = block(step)
        when(flag(to_pair), lambda: act(hand_key(owner)))
        for other, there in onward:
            when(flag(there), lambda: act(pass_key(owner, other)))

    def line_key(dist, act):
        there = (0 <= row + dist) & (row + dist < rows)
        straight = [abs(dist) == 1 or not chain for chain in CHAIN]
        if not all(straight):
            there = there & (second == straight.index(True)) if any(straight) else False
        when(there, lambda: act(own_key(me + 2 * dist)))

    def up_caches(act):
        for dist in range(1, rows):
            when(row - dist >= 0, lambda: act(own_cache(me - 2 * dist)))
            diagonal(CUP, -dist, True, lambda: act(own_cache(me - 2 * dist + 1 - 2 * side)))

    def down_caches(act):
        for dist in range(1, rows):
            when(row + dist < rows, lambda: act(own_cache(me + 2 * dist)))

    def at_step(places, step, act):
        if all(p == step for p in places):
            act()
        else:
            for g, p in enumerate(places):
                if p == step:
                    when(second == g, act)

    lines = [
        pick([[sorted((abs(r - z), r) for r in range(rows) if r != z)[i][1] for z in range(rows)]] * 2)
        for i in range(rows - 1)
    ]

    def handing(dist, act, other):
        there = row + dist < rows
        for g in range(2):
            when(there & (second == g), other if dist in CUP[g] else act)

    def caches(step):
        at_step(UP_AT, step, lambda: up_caches(lambda copy: copy.start()))
        at_step(DOWN_AT, step, lambda: down_caches(lambda copy: copy.start()))
        at_step(PAIR_AT, step, lambda: own_cache(pair).start())

        def here(peer):
            cache_copy(peer, peer, cs_sem.at[peer]).wait_recv()

        def hand(peer):
            here(peer)
            hand_cache(peer).start()

        for dist in range(1, rows):
            if HAND_UP[dist - 1] == step:
                handing(dist, lambda: hand(me + 2 * dist), lambda: here(me + 2 * dist))
            if HAND_DOWN[dist - 1] == step:
                when(row - dist >= 0, lambda: hand(me - 2 * dist))

    def partial(owner):
        for p in range(per):
            index = owner * per + p
            kb = keys[owner, p * BLK:(p + 1) * BLK, :]
            begin = start_ref[index]
            mask = jnp.where((position >= begin) & (position < begin + WIN), 1.0, 0.0)
            s = jnp.dot(kb, q_t[...], preferred_element_type=jnp.float32)
            top = jnp.max(s, axis=0, keepdims=True)
            e = jnp.exp2((s - top) * (scale * LOG2E))
            total = jnp.sum(e, axis=0, keepdims=True)
            acc = None
            for j in range(group):
                cols = slice(j * toks, (j + 1) * toks)
                term = e[:, cols] * (mask / total[:, cols])
                acc = term if acc is None else acc + term
            weight = jnp.sum(acc, axis=1, keepdims=True)
            rep = jnp.sum(weight * kb.astype(jnp.float32), axis=0, keepdims=True)
            mine[pl.ds(index, 1), :] = rep

    load_k.wait()

    when(side == 1, lambda: own_key(pair).start())
    for dist in reversed(range(1, rows)):
        line_key(-dist, lambda copy: copy.start())
    for dist in range(1, rows):
        diagonal(UP, -dist, side == 1, lambda: own_key(me - 2 * dist - 1).start())

    def later(dist):
        when(row + dist < rows, lambda: pl.semaphore_wait(ready.at[me + 2 * dist], 1))
        line_key(dist, lambda copy: copy.start())
        diagonal(DOWN, dist, side == 0, lambda: pl.semaphore_wait(ready.at[me + 2 * dist + 1], 1))
        diagonal(DOWN, dist, True, lambda: own_key(me + 2 * dist + 1 - 2 * side).start())

    def to_pair():
        pl.semaphore_wait(ready.at[pair], 1)
        own_key(pair).start()

    when(side == 0, to_pair)
    for dist in range(1, rows):
        diagonal(UP, -dist, side == 0, lambda: own_key(me - 2 * dist + 1).start())
    later(1)
    load_q.wait()
    load_w.wait()
    load_s.wait()
    for j in range(group):
        q_t[:, j * toks:(j + 1) * toks] = q_v[j].T
    position = me * toks + lax.broadcasted_iota(jnp.int32, (1, toks), 1)
    later(2)
    partial(me)
    for dist in range(3, rows):
        later(dist)
    load_c.wait()
    caches(-1)

    done = 0
    for step in range(n - 1):
        owner = block(step)[0]
        key_copy(owner, owner, ks_sem.at[owner]).wait_recv()
        relays(step, lambda copy: copy.start())
        caches(step)
        if step >= 3 - 1:
            for at in range(done, step + 1):
                partial(block(at)[0])
            done = step + 1

    each(n - 1, lambda i: part_copy(me, i + jnp.where(i >= me, 1, 0), mine).start())
    caches(n - 1)
    caches(n)
    cache_copy(pair, pair, cs_sem.at[pair]).wait_recv()
    for z in lines:
        owner = mate(z) + 1 - 2 * side
        cache_copy(owner, owner, cs_sem.at[owner]).wait_recv()
    hits = jnp.where(
        lax.broadcasted_iota(jnp.int32, (slots, blocks), 0) == slot_ref[...], 1.0, 0.0
    )
    taken = jnp.max(hits, axis=1, keepdims=True)
    hits = hits.astype(jnp.bfloat16)
    old = cache[...].reshape(slots, dim)

    each(n - 1, lambda i: part_copy(lax.rem(me + n - 1 - i, n), me, mine).wait_recv())
    parts[me] = mine[...]
    rep_sum = parts[0]
    for d in range(1, n):
        rep_sum = rep_sum + parts[d]
    rep = (rep_sum * (1.0 / (group * WIN))).astype(jnp.bfloat16)
    placed = jnp.dot(hits, rep, preferred_element_type=jnp.float32)
    bank[...] = jnp.where(taken > 0.5, placed, old.astype(jnp.float32)).astype(jnp.bfloat16)

    def sent(copy):
        copy.wait_send()

    sent(own_key(pair))
    sent(own_cache(pair))
    up_caches(sent)
    down_caches(sent)
    for dist in range(1, rows):
        for to, sets in ((-dist, UP), (dist, DOWN)):
            line_key(to, sent)
            diagonal(sets, to, True, lambda: sent(own_key(me + 2 * to + 1 - 2 * side)))
    for dist in range(1, rows):
        when(row - dist >= 0, lambda: sent(hand_cache(me - 2 * dist)))
        handing(dist, lambda: sent(hand_cache(me + 2 * dist)), lambda: None)
    for step in range(n - 1):
        relays(step, sent)
    each(n - 1, lambda i: sent(part_copy(me, i + jnp.where(i >= me, 1, 0), mine)))


def relate_kernel(q_v, bank, rel_hbm, bank_hbm, rel_v, sem):
    group, toks, dim = q_v.shape
    local = bank_hbm.shape[0]
    scale = 1.0 / math.sqrt(dim)
    first = pl.multiple_of(lax.axis_index("seq") * local, local)
    keep = pltpu.make_async_copy(bank.at[pl.ds(first, local)], bank_hbm, sem.at[group])
    keep.start()
    outs = [
        pltpu.make_async_copy(rel_v.at[j], rel_hbm.at[j], sem.at[j]) for j in range(group)
    ]
    for j in range(group):
        r = lax.dot_general(q_v[j], bank[...], NT, preferred_element_type=jnp.float32)
        rel_v[j] = (r * scale).astype(jnp.bfloat16)
        outs[j].start()
    for out in outs:
        out.wait()
    keep.wait()


def per_device(n, queries, new_keys, cache_keys, window_start, owner_slot):
    toks, group, dim = queries.shape
    ktoks, local = new_keys.shape[0], cache_keys.shape[0]
    blocks = window_start.shape[0]
    slots = n * local
    hbm_spec = pl.BlockSpec(memory_space=pltpu.HBM)
    vmem_spec = pl.BlockSpec(memory_space=pltpu.VMEM)
    bf16 = jnp.bfloat16
    short = n % 2 == 0 and n <= 8
    sems = [pltpu.SemaphoreType.DMA((n,))] * 6
    if short:
        sems = (
            [pltpu.SemaphoreType.REGULAR((n,))]
            + [pltpu.SemaphoreType.DMA((n,))] * 2
            + [pltpu.SemaphoreType.DMA((n * n // 2,))]
            + [pltpu.SemaphoreType.DMA((n,))] * 6
        )
    q_held, bank = pl.pallas_call(
        functools.partial(line_kernel if short else refresh_kernel, n),
        out_shape=(
            pltpu.VMEM((group, toks, dim), bf16),
            pltpu.VMEM((slots, dim), bf16),
        ),
        in_specs=[hbm_spec] * 5,
        out_specs=(vmem_spec, vmem_spec),
        scratch_shapes=[
            pltpu.SMEM((blocks,), jnp.int32),
            pltpu.VMEM((1, blocks), jnp.int32),
            pltpu.VMEM((dim, group * toks), bf16),
            pltpu.VMEM((n, ktoks, dim), bf16),
            pltpu.VMEM((n, local, dim), bf16),
            pltpu.VMEM((blocks, dim), jnp.float32),
            pltpu.VMEM((n, blocks, dim), jnp.float32),
            pltpu.SemaphoreType.DMA((5,)),
        ] + sems,
        compiler_params=pltpu.CompilerParams(
            collective_id=0, has_side_effects=True, vmem_limit_bytes=VMEM - 2 * dim * (group * toks + slots) - 16384
        ),
        name="refresh",
    )(
        window_start,
        owner_slot.reshape(1, blocks),
        jnp.transpose(queries, (1, 0, 2)),
        new_keys.reshape(ktoks, dim),
        cache_keys.reshape(local, dim),
    )
    rel, own = pl.pallas_call(
        relate_kernel,
        out_shape=(
            jax.ShapeDtypeStruct((group, toks, slots), bf16),
            jax.ShapeDtypeStruct((local, dim), bf16),
        ),
        in_specs=[vmem_spec, vmem_spec],
        out_specs=(hbm_spec, hbm_spec),
        scratch_shapes=[
            pltpu.VMEM((group, toks, slots), bf16),
            pltpu.SemaphoreType.DMA((group + 1,)),
        ],
        compiler_params=pltpu.CompilerParams(
            vmem_limit_bytes=2 * group * toks * slots + 16 * 1024 * 1024
        ),
        name="relate",
    )(q_held, bank)
    return jnp.transpose(rel, (1, 0, 2)), own[:, None, :]


def solution(mesh):
    spec = P("seq", "kvh", None)
    return jax.shard_map(
        functools.partial(per_device, mesh.shape["seq"]),
        mesh=mesh,
        in_specs=(spec, spec, spec, P(), P()),
        out_specs=(spec, spec),
        check_vma=False,
    )
```

```python
import functools
import math

import jax
import jax.numpy as jnp
from jax import lax
from jax.experimental import pallas as pl
from jax.experimental.pallas import tpu as pltpu
from jax.sharding import PartitionSpec as P

BLK = 128
WIN = 512
VMEM = 67043328
LOG2E = 1.4426950408889634
NT = (((1,), (1,)), ((), ()))


def each(count, body):
    if count <= 8:
        for i in range(count):
            body(i)
    else:
        lax.fori_loop(0, count, lambda i, c: (body(i), c)[1], 0)


def refresh_kernel(
    n, start_hbm, slot_hbm, q_hbm, k_hbm, c_hbm, q_v, bank,
    start_ref, slot_ref, q_t, keys, cache, mine, parts,
    load_sem, ks_sem, kr_sem, cs_sem, cr_sem, ps_sem, pr_sem,
):
    group, toks, dim = q_v.shape
    ktoks = keys.shape[1]
    local = cache.shape[1]
    slots = n * local
    per = ktoks // BLK
    blocks = n * per
    rows = group * toks
    scale = 1.0 / math.sqrt(dim)
    me = lax.axis_index("seq")

    load_k = pltpu.make_async_copy(k_hbm, keys.at[me], load_sem.at[0])
    load_q = pltpu.make_async_copy(q_hbm, q_v, load_sem.at[1])
    load_c = pltpu.make_async_copy(c_hbm, cache.at[me], load_sem.at[2])
    load_w = pltpu.make_async_copy(start_hbm, start_ref, load_sem.at[3])
    load_s = pltpu.make_async_copy(slot_hbm, slot_ref, load_sem.at[4])
    load_k.start()
    load_c.start()
    load_q.start()
    load_w.start()
    load_s.start()

    barrier = pltpu.get_barrier_semaphore()

    def greet(i):
        peer = lax.rem(me + 1 + i, n)
        pl.semaphore_signal(
            barrier, inc=1, device_id={"seq": peer}, device_id_type=pl.DeviceIdType.MESH
        )

    each(n - 1, greet)

    def link(src, dst, s_sem, r_sem, peer):
        return pltpu.make_async_remote_copy(
            src_ref=src, dst_ref=dst, send_sem=s_sem, recv_sem=r_sem,
            device_id={"seq": peer}, device_id_type=pl.DeviceIdType.MESH,
        )

    def key_copy(slot, peer):
        return link(keys.at[slot], keys.at[slot], ks_sem.at[peer], kr_sem.at[slot], peer)

    def cache_copy(slot, peer):
        return link(cache.at[slot], cache.at[slot], cs_sem.at[peer], cr_sem.at[slot], peer)

    def part_copy(slot, peer, src):
        return link(src, parts.at[slot], ps_sem.at[peer], pr_sem.at[slot], peer)

    load_q.wait()
    load_w.wait()
    load_s.wait()
    for j in range(group):
        q_t[:, j * toks:(j + 1) * toks] = q_v[j].T

    load_k.wait()
    position = me * toks + lax.broadcasted_iota(jnp.int32, (1, toks), 1)

    def partial(owner):
        for p in range(per):
            index = owner * per + p
            kb = keys[owner, p * BLK:(p + 1) * BLK, :]
            begin = start_ref[index]
            mask = jnp.where((position >= begin) & (position < begin + WIN), 1.0, 0.0)
            s = jnp.dot(kb, q_t[...], preferred_element_type=jnp.float32)
            top = jnp.max(s, axis=0, keepdims=True)
            e = jnp.exp2((s - top) * (scale * LOG2E))
            total = jnp.sum(e, axis=0, keepdims=True)
            acc = None
            for j in range(group):
                cols = slice(j * toks, (j + 1) * toks)
                term = e[:, cols] * (mask / total[:, cols])
                acc = term if acc is None else acc + term
            weight = jnp.sum(acc, axis=1, keepdims=True)
            rep = jnp.sum(weight * kb.astype(jnp.float32), axis=0, keepdims=True)
            mine[pl.ds(index, 1), :] = rep

    partial(me)

    pl.semaphore_wait(barrier, n - 1)
    each(n - 1, lambda i: key_copy(me, lax.rem(me + 1 + i, n)).start())
    load_c.wait()

    def arrive(i):
        owner = lax.rem(me + n - 1 - i, n)
        key_copy(owner, owner).wait_recv()
        partial(owner)

    each(n - 1, arrive)
    each(n - 1, lambda i: part_copy(me, lax.rem(me + 1 + i, n), mine).start())
    each(n - 1, lambda i: cache_copy(me, lax.rem(me + 1 + i, n)).start())

    each(n - 1, lambda i: cache_copy(lax.rem(me + n - 1 - i, n), me).wait_recv())
    hits = jnp.where(
        lax.broadcasted_iota(jnp.int32, (slots, blocks), 0) == slot_ref[...], 1.0, 0.0
    )
    taken = jnp.max(hits, axis=1, keepdims=True)
    hits = hits.astype(jnp.bfloat16)
    old = cache[...].reshape(slots, dim)

    each(n - 1, lambda i: part_copy(lax.rem(me + n - 1 - i, n), me, mine).wait_recv())
    parts[me] = mine[...]
    if n <= 8:
        rep_sum = parts[0]
        for d in range(1, n):
            rep_sum = rep_sum + parts[d]
    else:
        rep_sum = lax.fori_loop(1, n, lambda d, c: c + parts[d], parts[0])
    rep = (rep_sum * (1.0 / (group * WIN))).astype(jnp.bfloat16)
    placed = jnp.dot(hits, rep, preferred_element_type=jnp.float32)
    bank[...] = jnp.where(taken > 0.5, placed, old.astype(jnp.float32)).astype(jnp.bfloat16)
    def drain(i):
        peer = lax.rem(me + 1 + i, n)
        key_copy(me, peer).wait_send()
        cache_copy(me, peer).wait_send()
        part_copy(me, peer, mine).wait_send()

    each(n - 1, drain)


FAR = [2, 9]
COMPUTE_AT = [2, 3, 4, 5, 6]
UP = [(3,), ()]
CUP = [(1, 2, 3), ()]
DOWN = [(), ()]
T_DIAG = [0.8, 0.8]
CHAIN = [0, 0]
UP_AT = [2, 2]
DOWN_AT = [4, 4]
PAIR_AT = [3, 3]
HAND_UP = [7, 7, 7]
HAND_DOWN = [7, 7, 7]
T_PAIR = [4.0, 3.9]
T_LINE = [4.9, 4.0]
T_HOP = [0.9, 2.2]
T_RELAY = [3.2, 2.2]
T_FAR = [7.0, 9.0]


def plan(rows, group):
    far, chain = FAR[group], CHAIN[group]
    table = []

    def swaps(a, b):
        return b - a >= far and (b == rows - 1 or not 1)

    for z in range(rows):
        blocks = [(T_PAIR[group], z, 1, 0, tuple(r for r in range(rows) if swaps(z, r)))]
        for r in range(rows):
            if r == z:
                continue
            line = T_LINE[group] + T_HOP[group] * (abs(r - z) - 1)
            on = z + (1 if z > r else -1)
            straight = abs(r - z) in (DOWN if r < z else UP)[group] and (r > z or z == rows - 1 or not 0)
            blocks.append((line, r, 0, int(not swaps(r, z) and not straight), (on,) if chain and 0 <= on < rows else ()))
            other = line + (T_DIAG if straight else T_RELAY)[group]
            blocks.append((T_FAR[group] if swaps(r, z) else other, r, 1, 0, ()))
        table.append([b[1:] for b in sorted(blocks)])
    return table


def line_kernel(
    n, start_hbm, slot_hbm, q_hbm, k_hbm, c_hbm, q_v, bank,
    start_ref, slot_ref, q_t, keys, cache, mine, parts,
    load_sem, ready, ks_sem, kf_sem, kl_sem, kr_sem, cs_sem, cf_sem, cr_sem, ps_sem, pr_sem,
):
    group, toks, dim = q_v.shape
    ktoks = keys.shape[1]
    local = cache.shape[1]
    slots = n * local
    per = ktoks // BLK
    blocks = n * per
    rows = n // 2
    scale = 1.0 / math.sqrt(dim)
    me = lax.axis_index("seq")
    second = lax.axis_index("kvh") % 2
    row = me // 2
    side = me % 2
    pair = me + 1 - 2 * side

    load_k = pltpu.make_async_copy(k_hbm, keys.at[me], load_sem.at[0])
    load_q = pltpu.make_async_copy(q_hbm, q_v, load_sem.at[1])
    load_c = pltpu.make_async_copy(c_hbm, cache.at[me], load_sem.at[2])
    load_w = pltpu.make_async_copy(start_hbm, start_ref, load_sem.at[3])
    load_s = pltpu.make_async_copy(slot_hbm, slot_ref, load_sem.at[4])
    load_k.start()

    barrier = pltpu.get_barrier_semaphore()

    def signal(sem, peer):
        pl.semaphore_signal(
            sem, inc=1, device_id={"seq": peer}, device_id_type=pl.DeviceIdType.MESH
        )

    def when(flag, act):
        if isinstance(flag, (bool, int)):
            if flag:
                act()
        else:
            pl.when(flag)(act)

    def mate(other):
        return 2 * other + side

    when(side == 0, lambda: signal(barrier, pair))
    for other in range(1, rows):
        when(other > row, lambda: signal(barrier, mate(other)))

    def diagonal(sets, dist, there, act):
        there = (0 <= row + dist) & (row + dist < rows) & there
        if 0 and sets is DOWN:
            there = there & ((row == rows - 1) if dist < 0 else (row + dist == rows - 1))
        has = [abs(dist) in g for g in sets]
        if any(has):
            when(there if all(has) else there & (second == has.index(True)), act)

    both = [set(a) | set(b) | set(c) for a, b, c in zip(UP, DOWN, CUP)]
    for dist in range(1, rows):
        diagonal(both, dist, side == 0, lambda: signal(barrier, me + 2 * dist + 1))

    load_q.start()
    load_c.start()
    load_w.start()
    load_s.start()

    count = row + side
    for g in range(2):
        for dist in sorted(both[g]):
            count = count + jnp.where((side == 1) & (row >= dist) & (second == g), 1, 0)

    when(me > 0, lambda: pl.semaphore_wait(barrier, count))
    when(side == 1, lambda: signal(ready.at[me], pair))
    for other in reversed(range(rows - 1)):
        when(other < row, lambda: signal(ready.at[me], mate(other)))
    for dist in reversed(range(1, rows)):
        diagonal(DOWN, -dist, side == 1, lambda: signal(ready.at[me], me - 2 * dist - 1))

    def link(src, dst, s_sem, r_sem, peer):
        return pltpu.make_async_remote_copy(
            src_ref=src, dst_ref=dst, send_sem=s_sem, recv_sem=r_sem,
            device_id={"seq": peer}, device_id_type=pl.DeviceIdType.MESH,
        )

    def key_copy(slot, peer, sem):
        return link(keys.at[slot], keys.at[slot], sem, kr_sem.at[slot], peer)

    def cache_copy(slot, peer, sem):
        return link(cache.at[slot], cache.at[slot], sem, cr_sem.at[slot], peer)

    def part_copy(slot, peer, src):
        return link(src, parts.at[slot], ps_sem.at[peer], pr_sem.at[slot], peer)

    def own_key(peer):
        return key_copy(me, peer, ks_sem.at[peer])

    def own_cache(peer):
        return cache_copy(me, peer, cs_sem.at[peer])

    def hand_key(owner):
        return key_copy(owner, pair, kf_sem.at[owner])

    def pass_key(owner, other):
        return key_copy(owner, mate(other), kl_sem.at[owner * rows + other])

    def hand_cache(owner):
        return cache_copy(owner, pair, cf_sem.at[owner])

    def pick(values):
        flat = [v for group in values for v in group]
        if len(set(flat)) == 1:
            return flat[0]
        out = flat[0]
        for at, v in enumerate(flat):
            if v != flat[0]:
                out = jnp.where(second * rows + row == at, v, out)
        return out

    tables = [plan(rows, g) for g in range(2)]

    def block(step):
        z, cross, to_pair = (
            pick([[t[r][step][i] for r in range(rows)] for t in tables]) for i in range(3)
        )
        onward = [
            (other, pick([[int(other in t[r][step][3]) for r in range(rows)] for t in tables]))
            for other in range(rows)
        ]
        return mate(z) + cross * (1 - 2 * side), to_pair, onward

    def flag(value):
        return bool(value) if isinstance(value, int) else value == 1

    def relays(step, act):
        owner, to_pair, onward = block(step)
        when(flag(to_pair), lambda: act(hand_key(owner)))
        for other, there in onward:
            when(flag(there), lambda: act(pass_key(owner, other)))

    def line_key(dist, act):
        there = (0 <= row + dist) & (row + dist < rows)
        straight = [abs(dist) == 1 or not chain for chain in CHAIN]
        if not all(straight):
            there = there & (second == straight.index(True)) if any(straight) else False
        when(there, lambda: act(own_key(me + 2 * dist)))

    def up_caches(act):
        for dist in range(1, rows):
            when(row - dist >= 0, lambda: act(own_cache(me - 2 * dist)))
            diagonal(CUP, -dist, True, lambda: act(own_cache(me - 2 * dist + 1 - 2 * side)))

    def down_caches(act):
        for dist in range(1, rows):
            when(row + dist < rows, lambda: act(own_cache(me + 2 * dist)))

    def at_step(places, step, act):
        if all(p == step for p in places):
            act()
        else:
            for g, p in enumerate(places):
                if p == step:
                    when(second == g, act)

    lines = [
        pick([[sorted((abs(r - z), r) for r in range(rows) if r != z)[i][1] for z in range(rows)]] * 2)
        for i in range(rows - 1)
    ]

    def handing(dist, act, other):
        there = row + dist < rows
        for g in range(2):
            when(there & (second == g), other if dist in CUP[g] else act)

    def caches(step):
        at_step(UP_AT, step, lambda: up_caches(lambda copy: copy.start()))
        at_step(DOWN_AT, step, lambda: down_caches(lambda copy: copy.start()))
        at_step(PAIR_AT, step, lambda: own_cache(pair).start())

        def here(peer):
            cache_copy(peer, peer, cs_sem.at[peer]).wait_recv()

        def hand(peer):
            here(peer)
            hand_cache(peer).start()

        for dist in range(1, rows):
            if HAND_UP[dist - 1] == step:
                handing(dist, lambda: hand(me + 2 * dist), lambda: here(me + 2 * dist))
            if HAND_DOWN[dist - 1] == step:
                when(row - dist >= 0, lambda: hand(me - 2 * dist))

    def partial(owner):
        for p in range(per):
            index = owner * per + p
            kb = keys[owner, p * BLK:(p + 1) * BLK, :]
            begin = start_ref[index]
            mask = jnp.where((position >= begin) & (position < begin + WIN), 1.0, 0.0)
            s = jnp.dot(kb, q_t[...], preferred_element_type=jnp.float32)
            top = jnp.max(s, axis=0, keepdims=True)
            e = jnp.exp2((s - top) * (scale * LOG2E))
            total = jnp.sum(e, axis=0, keepdims=True)
            acc = None
            for j in range(group):
                cols = slice(j * toks, (j + 1) * toks)
                term = e[:, cols] * (mask / total[:, cols])
                acc = term if acc is None else acc + term
            weight = jnp.sum(acc, axis=1, keepdims=True)
            rep = jnp.sum(weight * kb.astype(jnp.float32), axis=0, keepdims=True)
            mine[pl.ds(index, 1), :] = rep

    load_k.wait()

    when(side == 1, lambda: own_key(pair).start())
    for dist in reversed(range(1, rows)):
        line_key(-dist, lambda copy: copy.start())
    for dist in range(1, rows):
        diagonal(UP, -dist, side == 1, lambda: own_key(me - 2 * dist - 1).start())

    def later(dist):
        when(row + dist < rows, lambda: pl.semaphore_wait(ready.at[me + 2 * dist], 1))
        line_key(dist, lambda copy: copy.start())
        diagonal(DOWN, dist, side == 0, lambda: pl.semaphore_wait(ready.at[me + 2 * dist + 1], 1))
        diagonal(DOWN, dist, True, lambda: own_key(me + 2 * dist + 1 - 2 * side).start())

    def to_pair():
        pl.semaphore_wait(ready.at[pair], 1)
        own_key(pair).start()

    when(side == 0, to_pair)
    for dist in range(1, rows):
        diagonal(UP, -dist, side == 0, lambda: own_key(me - 2 * dist + 1).start())
    later(1)
    load_q.wait()
    load_w.wait()
    load_s.wait()
    for j in range(group):
        q_t[:, j * toks:(j + 1) * toks] = q_v[j].T
    position = me * toks + lax.broadcasted_iota(jnp.int32, (1, toks), 1)
    later(2)
    partial(me)
    for dist in range(3, rows):
        later(dist)
    load_c.wait()
    caches(-1)

    done = 0
    for step in range(n - 1):
        owner = block(step)[0]
        key_copy(owner, owner, ks_sem.at[owner]).wait_recv()
        relays(step, lambda copy: copy.start())
        caches(step)
        if step in COMPUTE_AT:
            for at in range(done, step + 1):
                partial(block(at)[0])
            done = step + 1

    each(n - 1, lambda i: part_copy(me, i + jnp.where(i >= me, 1, 0), mine).start())
    caches(n - 1)
    caches(n)
    cache_copy(pair, pair, cs_sem.at[pair]).wait_recv()
    for z in lines:
        owner = mate(z) + 1 - 2 * side
        cache_copy(owner, owner, cs_sem.at[owner]).wait_recv()
    hits = jnp.where(
        lax.broadcasted_iota(jnp.int32, (slots, blocks), 0) == slot_ref[...], 1.0, 0.0
    )
    taken = jnp.max(hits, axis=1, keepdims=True)
    hits = hits.astype(jnp.bfloat16)
    old = cache[...].reshape(slots, dim)

    each(n - 1, lambda i: part_copy(lax.rem(me + n - 1 - i, n), me, mine).wait_recv())
    parts[me] = mine[...]
    rep_sum = parts[0]
    for d in range(1, n):
        rep_sum = rep_sum + parts[d]
    rep = (rep_sum * (1.0 / (group * WIN))).astype(jnp.bfloat16)
    placed = jnp.dot(hits, rep, preferred_element_type=jnp.float32)
    bank[...] = jnp.where(taken > 0.5, placed, old.astype(jnp.float32)).astype(jnp.bfloat16)

    def sent(copy):
        copy.wait_send()

    sent(own_key(pair))
    sent(own_cache(pair))
    up_caches(sent)
    down_caches(sent)
    for dist in range(1, rows):
        for to, sets in ((-dist, UP), (dist, DOWN)):
            line_key(to, sent)
            diagonal(sets, to, True, lambda: sent(own_key(me + 2 * to + 1 - 2 * side)))
    for dist in range(1, rows):
        when(row - dist >= 0, lambda: sent(hand_cache(me - 2 * dist)))
        handing(dist, lambda: sent(hand_cache(me + 2 * dist)), lambda: None)
    for step in range(n - 1):
        relays(step, sent)
    each(n - 1, lambda i: sent(part_copy(me, i + jnp.where(i >= me, 1, 0), mine)))


def relate_kernel(q_v, bank, rel_hbm, bank_hbm, rel_v, sem):
    group, toks, dim = q_v.shape
    local = bank_hbm.shape[0]
    scale = 1.0 / math.sqrt(dim)
    first = pl.multiple_of(lax.axis_index("seq") * local, local)
    keep = pltpu.make_async_copy(bank.at[pl.ds(first, local)], bank_hbm, sem.at[group])
    keep.start()
    outs = [
        pltpu.make_async_copy(rel_v.at[j], rel_hbm.at[j], sem.at[j]) for j in range(group)
    ]
    for j in range(group):
        r = lax.dot_general(q_v[j], bank[...], NT, preferred_element_type=jnp.float32)
        rel_v[j] = (r * scale).astype(jnp.bfloat16)
        outs[j].start()
    for out in outs:
        out.wait()
    keep.wait()


def per_device(n, queries, new_keys, cache_keys, window_start, owner_slot):
    toks, group, dim = queries.shape
    ktoks, local = new_keys.shape[0], cache_keys.shape[0]
    blocks = window_start.shape[0]
    slots = n * local
    hbm_spec = pl.BlockSpec(memory_space=pltpu.HBM)
    vmem_spec = pl.BlockSpec(memory_space=pltpu.VMEM)
    bf16 = jnp.bfloat16
    short = n % 2 == 0 and n <= 8
    sems = [pltpu.SemaphoreType.DMA((n,))] * 6
    if short:
        sems = (
            [pltpu.SemaphoreType.REGULAR((n,))]
            + [pltpu.SemaphoreType.DMA((n,))] * 2
            + [pltpu.SemaphoreType.DMA((n * n // 2,))]
            + [pltpu.SemaphoreType.DMA((n,))] * 6
        )
    q_held, bank = pl.pallas_call(
        functools.partial(line_kernel if short else refresh_kernel, n),
        out_shape=(
            pltpu.VMEM((group, toks, dim), bf16),
            pltpu.VMEM((slots, dim), bf16),
        ),
        in_specs=[hbm_spec] * 5,
        out_specs=(vmem_spec, vmem_spec),
        scratch_shapes=[
            pltpu.SMEM((blocks,), jnp.int32),
            pltpu.VMEM((1, blocks), jnp.int32),
            pltpu.VMEM((dim, group * toks), bf16),
            pltpu.VMEM((n, ktoks, dim), bf16),
            pltpu.VMEM((n, local, dim), bf16),
            pltpu.VMEM((blocks, dim), jnp.float32),
            pltpu.VMEM((n, blocks, dim), jnp.float32),
            pltpu.SemaphoreType.DMA((5,)),
        ] + sems,
        compiler_params=pltpu.CompilerParams(
            collective_id=0, has_side_effects=True, vmem_limit_bytes=VMEM - 2 * dim * (group * toks + slots) - 16384
        ),
        name="refresh",
    )(
        window_start,
        owner_slot.reshape(1, blocks),
        jnp.transpose(queries, (1, 0, 2)),
        new_keys.reshape(ktoks, dim),
        cache_keys.reshape(local, dim),
    )
    rel, own = pl.pallas_call(
        relate_kernel,
        out_shape=(
            jax.ShapeDtypeStruct((group, toks, slots), bf16),
            jax.ShapeDtypeStruct((local, dim), bf16),
        ),
        in_specs=[vmem_spec, vmem_spec],
        out_specs=(hbm_spec, hbm_spec),
        scratch_shapes=[
            pltpu.VMEM((group, toks, slots), bf16),
            pltpu.SemaphoreType.DMA((group + 1,)),
        ],
        compiler_params=pltpu.CompilerParams(
            vmem_limit_bytes=2 * group * toks * slots + 16 * 1024 * 1024
        ),
        name="relate",
    )(q_held, bank)
    return jnp.transpose(rel, (1, 0, 2)), own[:, None, :]


def solution(mesh):
    spec = P("seq", "kvh", None)
    return jax.shard_map(
        functools.partial(per_device, mesh.shape["seq"]),
        mesh=mesh,
        in_specs=(spec, spec, spec, P(), P()),
        out_specs=(spec, spec),
        check_vma=False,
    )
```

```python
import functools
import math

import jax
import jax.numpy as jnp
from jax import lax
from jax.experimental import pallas as pl
from jax.experimental.pallas import tpu as pltpu
from jax.sharding import PartitionSpec as P

BLK = 128
WIN = 512
VMEM = 67043328
LOG2E = 1.4426950408889634
NT = (((1,), (1,)), ((), ()))


def each(count, body):
    if count <= 8:
        for i in range(count):
            body(i)
    else:
        lax.fori_loop(0, count, lambda i, c: (body(i), c)[1], 0)


def refresh_kernel(
    n, start_hbm, slot_hbm, q_hbm, k_hbm, c_hbm, q_v, bank,
    start_ref, slot_ref, q_t, keys, cache, mine, parts,
    load_sem, ks_sem, kr_sem, cs_sem, cr_sem, ps_sem, pr_sem,
):
    group, toks, dim = q_v.shape
    ktoks = keys.shape[1]
    local = cache.shape[1]
    slots = n * local
    per = ktoks // BLK
    blocks = n * per
    rows = group * toks
    scale = 1.0 / math.sqrt(dim)
    me = lax.axis_index("seq")

    load_k = pltpu.make_async_copy(k_hbm, keys.at[me], load_sem.at[0])
    load_q = pltpu.make_async_copy(q_hbm, q_v, load_sem.at[1])
    load_c = pltpu.make_async_copy(c_hbm, cache.at[me], load_sem.at[2])
    load_w = pltpu.make_async_copy(start_hbm, start_ref, load_sem.at[3])
    load_s = pltpu.make_async_copy(slot_hbm, slot_ref, load_sem.at[4])
    load_k.start()
    load_c.start()
    load_q.start()
    load_w.start()
    load_s.start()

    barrier = pltpu.get_barrier_semaphore()

    def greet(i):
        peer = lax.rem(me + 1 + i, n)
        pl.semaphore_signal(
            barrier, inc=1, device_id={"seq": peer}, device_id_type=pl.DeviceIdType.MESH
        )

    each(n - 1, greet)

    def link(src, dst, s_sem, r_sem, peer):
        return pltpu.make_async_remote_copy(
            src_ref=src, dst_ref=dst, send_sem=s_sem, recv_sem=r_sem,
            device_id={"seq": peer}, device_id_type=pl.DeviceIdType.MESH,
        )

    def key_copy(slot, peer):
        return link(keys.at[slot], keys.at[slot], ks_sem.at[peer], kr_sem.at[slot], peer)

    def cache_copy(slot, peer):
        return link(cache.at[slot], cache.at[slot], cs_sem.at[peer], cr_sem.at[slot], peer)

    def part_copy(slot, peer, src):
        return link(src, parts.at[slot], ps_sem.at[peer], pr_sem.at[slot], peer)

    load_q.wait()
    load_w.wait()
    load_s.wait()
    for j in range(group):
        q_t[:, j * toks:(j + 1) * toks] = q_v[j].T

    load_k.wait()
    position = me * toks + lax.broadcasted_iota(jnp.int32, (1, toks), 1)

    def partial(owner):
        for p in range(per):
            index = owner * per + p
            kb = keys[owner, p * BLK:(p + 1) * BLK, :]
            begin = start_ref[index]
            mask = jnp.where((position >= begin) & (position < begin + WIN), 1.0, 0.0)
            s = jnp.dot(kb, q_t[...], preferred_element_type=jnp.float32)
            top = jnp.max(s, axis=0, keepdims=True)
            e = jnp.exp2((s - top) * (scale * LOG2E))
            total = jnp.sum(e, axis=0, keepdims=True)
            acc = None
            for j in range(group):
                cols = slice(j * toks, (j + 1) * toks)
                term = e[:, cols] * (mask / total[:, cols])
                acc = term if acc is None else acc + term
            weight = jnp.sum(acc, axis=1, keepdims=True)
            rep = jnp.sum(weight * kb.astype(jnp.float32), axis=0, keepdims=True)
            mine[pl.ds(index, 1), :] = rep

    partial(me)

    pl.semaphore_wait(barrier, n - 1)
    each(n - 1, lambda i: key_copy(me, lax.rem(me + 1 + i, n)).start())
    load_c.wait()

    def arrive(i):
        owner = lax.rem(me + n - 1 - i, n)
        key_copy(owner, owner).wait_recv()
        partial(owner)

    each(n - 1, arrive)
    each(n - 1, lambda i: part_copy(me, lax.rem(me + 1 + i, n), mine).start())
    each(n - 1, lambda i: cache_copy(me, lax.rem(me + 1 + i, n)).start())

    each(n - 1, lambda i: cache_copy(lax.rem(me + n - 1 - i, n), me).wait_recv())
    hits = jnp.where(
        lax.broadcasted_iota(jnp.int32, (slots, blocks), 0) == slot_ref[...], 1.0, 0.0
    )
    taken = jnp.max(hits, axis=1, keepdims=True)
    hits = hits.astype(jnp.bfloat16)
    old = cache[...].reshape(slots, dim)

    each(n - 1, lambda i: part_copy(lax.rem(me + n - 1 - i, n), me, mine).wait_recv())
    parts[me] = mine[...]
    if n <= 8:
        rep_sum = parts[0]
        for d in range(1, n):
            rep_sum = rep_sum + parts[d]
    else:
        rep_sum = lax.fori_loop(1, n, lambda d, c: c + parts[d], parts[0])
    rep = (rep_sum * (1.0 / (group * WIN))).astype(jnp.bfloat16)
    placed = jnp.dot(hits, rep, preferred_element_type=jnp.float32)
    bank[...] = jnp.where(taken > 0.5, placed, old.astype(jnp.float32)).astype(jnp.bfloat16)
    def drain(i):
        peer = lax.rem(me + 1 + i, n)
        key_copy(me, peer).wait_send()
        cache_copy(me, peer).wait_send()
        part_copy(me, peer, mine).wait_send()

    each(n - 1, drain)


FAR = [2, 9]
UP = [(3,), ()]
CUP = [(1, 2, 3), ()]
DOWN = [(), ()]
T_DIAG = [0.8, 0.8]
CHAIN = [0, 0]
UP_AT = [2, 2]
DOWN_AT = [4, 4]
PAIR_AT = [3, 3]
HAND_UP = [7, 7, 7]
HAND_DOWN = [7, 7, 7]
T_PAIR = [4.0, 3.9]
T_LINE = [4.9, 4.0]
T_HOP = [0.9, 2.2]
T_RELAY = [3.2, 2.2]
T_FAR = [7.0, 9.0]


def plan(rows, group):
    far, chain = FAR[group], CHAIN[group]
    table = []

    def swaps(a, b):
        return b - a >= far and (b == rows - 1 or not 1)

    for z in range(rows):
        blocks = [(T_PAIR[group], z, 1, 0, tuple(r for r in range(rows) if swaps(z, r)))]
        for r in range(rows):
            if r == z:
                continue
            line = T_LINE[group] + T_HOP[group] * (abs(r - z) - 1)
            on = z + (1 if z > r else -1)
            straight = abs(r - z) in (DOWN if r < z else UP)[group] and (r > z or z == rows - 1 or not 0)
            blocks.append((line, r, 0, int(not swaps(r, z) and not straight), (on,) if chain and 0 <= on < rows else ()))
            other = line + (T_DIAG if straight else T_RELAY)[group]
            blocks.append((T_FAR[group] if swaps(r, z) else other, r, 1, 0, ()))
        table.append([b[1:] for b in sorted(blocks)])
    return table


def line_kernel(
    n, start_hbm, slot_hbm, q_hbm, k_hbm, c_hbm, q_v, bank,
    start_ref, slot_ref, q_t, keys, cache, mine, parts,
    load_sem, ready, ks_sem, kf_sem, kl_sem, kr_sem, cs_sem, cf_sem, cr_sem, ps_sem, pr_sem,
):
    group, toks, dim = q_v.shape
    ktoks = keys.shape[1]
    local = cache.shape[1]
    slots = n * local
    per = ktoks // BLK
    blocks = n * per
    rows = n // 2
    scale = 1.0 / math.sqrt(dim)
    me = lax.axis_index("seq")
    second = lax.axis_index("kvh") % 2
    row = me // 2
    side = me % 2
    pair = me + 1 - 2 * side

    load_k = pltpu.make_async_copy(k_hbm, keys.at[me], load_sem.at[0])
    load_q = pltpu.make_async_copy(q_hbm, q_v, load_sem.at[1])
    load_c = pltpu.make_async_copy(c_hbm, cache.at[me], load_sem.at[2])
    load_w = pltpu.make_async_copy(start_hbm, start_ref, load_sem.at[3])
    load_s = pltpu.make_async_copy(slot_hbm, slot_ref, load_sem.at[4])
    load_k.start()
    load_q.start()
    load_c.start()
    load_w.start()
    load_s.start()

    barrier = pltpu.get_barrier_semaphore()

    def signal(sem, peer):
        pl.semaphore_signal(
            sem, inc=1, device_id={"seq": peer}, device_id_type=pl.DeviceIdType.MESH
        )

    def when(flag, act):
        if isinstance(flag, (bool, int)):
            if flag:
                act()
        else:
            pl.when(flag)(act)

    def mate(other):
        return 2 * other + side

    when(side == 0, lambda: signal(barrier, pair))
    for other in range(1, rows):
        when(other > row, lambda: signal(barrier, mate(other)))

    def diagonal(sets, dist, there, act):
        there = (0 <= row + dist) & (row + dist < rows) & there
        if 0 and sets is DOWN:
            there = there & ((row == rows - 1) if dist < 0 else (row + dist == rows - 1))
        has = [abs(dist) in g for g in sets]
        if any(has):
            when(there if all(has) else there & (second == has.index(True)), act)

    both = [set(a) | set(b) | set(c) for a, b, c in zip(UP, DOWN, CUP)]
    for dist in range(1, rows):
        diagonal(both, dist, side == 0, lambda: signal(barrier, me + 2 * dist + 1))

    count = row + side
    for g in range(2):
        for dist in sorted(both[g]):
            count = count + jnp.where((side == 1) & (row >= dist) & (second == g), 1, 0)

    when(me > 0, lambda: pl.semaphore_wait(barrier, count))
    when(side == 1, lambda: signal(ready.at[me], pair))
    for other in reversed(range(rows - 1)):
        when(other < row, lambda: signal(ready.at[me], mate(other)))
    for dist in reversed(range(1, rows)):
        diagonal(DOWN, -dist, side == 1, lambda: signal(ready.at[me], me - 2 * dist - 1))

    def link(src, dst, s_sem, r_sem, peer):
        return pltpu.make_async_remote_copy(
            src_ref=src, dst_ref=dst, send_sem=s_sem, recv_sem=r_sem,
            device_id={"seq": peer}, device_id_type=pl.DeviceIdType.MESH,
        )

    def key_copy(slot, peer, sem):
        return link(keys.at[slot], keys.at[slot], sem, kr_sem.at[slot], peer)

    def cache_copy(slot, peer, sem):
        return link(cache.at[slot], cache.at[slot], sem, cr_sem.at[slot], peer)

    def part_copy(slot, peer, src):
        return link(src, parts.at[slot], ps_sem.at[peer], pr_sem.at[slot], peer)

    def own_key(peer):
        return key_copy(me, peer, ks_sem.at[peer])

    def own_cache(peer):
        return cache_copy(me, peer, cs_sem.at[peer])

    def hand_key(owner):
        return key_copy(owner, pair, kf_sem.at[owner])

    def pass_key(owner, other):
        return key_copy(owner, mate(other), kl_sem.at[owner * rows + other])

    def hand_cache(owner):
        return cache_copy(owner, pair, cf_sem.at[owner])

    def pick(values):
        flat = [v for group in values for v in group]
        if len(set(flat)) == 1:
            return flat[0]
        out = flat[0]
        for at, v in enumerate(flat):
            if v != flat[0]:
                out = jnp.where(second * rows + row == at, v, out)
        return out

    tables = [plan(rows, g) for g in range(2)]

    def block(step):
        z, cross, to_pair = (
            pick([[t[r][step][i] for r in range(rows)] for t in tables]) for i in range(3)
        )
        onward = [
            (other, pick([[int(other in t[r][step][3]) for r in range(rows)] for t in tables]))
            for other in range(rows)
        ]
        return mate(z) + cross * (1 - 2 * side), to_pair, onward

    def flag(value):
        return bool(value) if isinstance(value, int) else value == 1

    def relays(step, act):
        owner, to_pair, onward = block(step)
        when(flag(to_pair), lambda: act(hand_key(owner)))
        for other, there in onward:
            when(flag(there), lambda: act(pass_key(owner, other)))

    def line_key(dist, act):
        there = (0 <= row + dist) & (row + dist < rows)
        straight = [abs(dist) == 1 or not chain for chain in CHAIN]
        if not all(straight):
            there = there & (second == straight.index(True)) if any(straight) else False
        when(there, lambda: act(own_key(me + 2 * dist)))

    def up_caches(act):
        for dist in range(1, rows):
            when(row - dist >= 0, lambda: act(own_cache(me - 2 * dist)))
            diagonal(CUP, -dist, True, lambda: act(own_cache(me - 2 * dist + 1 - 2 * side)))

    def down_caches(act):
        for dist in range(1, rows):
            when(row + dist < rows, lambda: act(own_cache(me + 2 * dist)))

    def at_step(places, step, act):
        if all(p == step for p in places):
            act()
        else:
            for g, p in enumerate(places):
                if p == step:
                    when(second == g, act)

    lines = [
        pick([[sorted((abs(r - z), r) for r in range(rows) if r != z)[i][1] for z in range(rows)]] * 2)
        for i in range(rows - 1)
    ]

    def handing(dist, act, other):
        there = row + dist < rows
        for g in range(2):
            when(there & (second == g), other if dist in CUP[g] else act)

    def caches(step):
        at_step(UP_AT, step, lambda: up_caches(lambda copy: copy.start()))
        at_step(DOWN_AT, step, lambda: down_caches(lambda copy: copy.start()))
        at_step(PAIR_AT, step, lambda: own_cache(pair).start())

        def here(peer):
            cache_copy(peer, peer, cs_sem.at[peer]).wait_recv()

        def hand(peer):
            here(peer)
            hand_cache(peer).start()

        for dist in range(1, rows):
            if HAND_UP[dist - 1] == step:
                handing(dist, lambda: hand(me + 2 * dist), lambda: here(me + 2 * dist))
            if HAND_DOWN[dist - 1] == step:
                when(row - dist >= 0, lambda: hand(me - 2 * dist))

    def partial(owner):
        for p in range(per):
            index = owner * per + p
            kb = keys[owner, p * BLK:(p + 1) * BLK, :]
            begin = start_ref[index]
            mask = jnp.where((position >= begin) & (position < begin + WIN), 1.0, 0.0)
            s = jnp.dot(kb, q_t[...], preferred_element_type=jnp.float32)
            top = jnp.max(s, axis=0, keepdims=True)
            e = jnp.exp2((s - top) * (scale * LOG2E))
            total = jnp.sum(e, axis=0, keepdims=True)
            acc = None
            for j in range(group):
                cols = slice(j * toks, (j + 1) * toks)
                term = e[:, cols] * (mask / total[:, cols])
                acc = term if acc is None else acc + term
            weight = jnp.sum(acc, axis=1, keepdims=True)
            rep = jnp.sum(weight * kb.astype(jnp.float32), axis=0, keepdims=True)
            mine[pl.ds(index, 1), :] = rep

    load_k.wait()

    when(side == 1, lambda: own_key(pair).start())
    for dist in reversed(range(1, rows)):
        line_key(-dist, lambda copy: copy.start())
    for dist in range(1, rows):
        diagonal(UP, -dist, side == 1, lambda: own_key(me - 2 * dist - 1).start())

    def later(dist):
        when(row + dist < rows, lambda: pl.semaphore_wait(ready.at[me + 2 * dist], 1))
        line_key(dist, lambda copy: copy.start())
        diagonal(DOWN, dist, side == 0, lambda: pl.semaphore_wait(ready.at[me + 2 * dist + 1], 1))
        diagonal(DOWN, dist, True, lambda: own_key(me + 2 * dist + 1 - 2 * side).start())

    def to_pair():
        pl.semaphore_wait(ready.at[pair], 1)
        own_key(pair).start()

    when(side == 0, to_pair)
    for dist in range(1, rows):
        diagonal(UP, -dist, side == 0, lambda: own_key(me - 2 * dist + 1).start())
    later(1)
    load_q.wait()
    load_w.wait()
    load_s.wait()
    for j in range(group):
        q_t[:, j * toks:(j + 1) * toks] = q_v[j].T
    position = me * toks + lax.broadcasted_iota(jnp.int32, (1, toks), 1)
    later(2)
    partial(me)
    for dist in range(3, rows):
        later(dist)
    load_c.wait()
    caches(-1)

    done = 0
    for step in range(n - 1):
        owner = block(step)[0]
        key_copy(owner, owner, ks_sem.at[owner]).wait_recv()
        relays(step, lambda copy: copy.start())
        caches(step)
        if step >= 3 - 1:
            for at in range(done, step + 1):
                partial(block(at)[0])
            done = step + 1

    each(n - 1, lambda i: part_copy(me, i + jnp.where(i >= me, 1, 0), mine).start())
    caches(n - 1)
    caches(n)
    cache_copy(pair, pair, cs_sem.at[pair]).wait_recv()
    for z in lines:
        owner = mate(z) + 1 - 2 * side
        cache_copy(owner, owner, cs_sem.at[owner]).wait_recv()
    hits = jnp.where(
        lax.broadcasted_iota(jnp.int32, (slots, blocks), 0) == slot_ref[...], 1.0, 0.0
    )
    taken = jnp.max(hits, axis=1, keepdims=True)
    hits = hits.astype(jnp.bfloat16)
    old = cache[...].reshape(slots, dim)

    each(n - 1, lambda i: part_copy(lax.rem(me + n - 1 - i, n), me, mine).wait_recv())
    parts[me] = mine[...]
    rep_sum = parts[0]
    for d in range(1, n):
        rep_sum = rep_sum + parts[d]
    rep = (rep_sum * (1.0 / (group * WIN))).astype(jnp.bfloat16)
    placed = jnp.dot(hits, rep, preferred_element_type=jnp.float32)
    bank[...] = jnp.where(taken > 0.5, placed, old.astype(jnp.float32)).astype(jnp.bfloat16)

    def sent(copy):
        copy.wait_send()

    sent(own_key(pair))
    sent(own_cache(pair))
    up_caches(sent)
    down_caches(sent)
    for dist in range(1, rows):
        for to, sets in ((-dist, UP), (dist, DOWN)):
            line_key(to, sent)
            diagonal(sets, to, True, lambda: sent(own_key(me + 2 * to + 1 - 2 * side)))
    for dist in range(1, rows):
        when(row - dist >= 0, lambda: sent(hand_cache(me - 2 * dist)))
        handing(dist, lambda: sent(hand_cache(me + 2 * dist)), lambda: None)
    for step in range(n - 1):
        relays(step, sent)
    each(n - 1, lambda i: sent(part_copy(me, i + jnp.where(i >= me, 1, 0), mine)))


def relate_kernel(q_v, bank, rel_hbm, bank_hbm, rel_v, sem):
    group, toks, dim = q_v.shape
    local = bank_hbm.shape[0]
    half = toks // 2
    scale = 1.0 / math.sqrt(dim)
    first = pl.multiple_of(lax.axis_index("seq") * local, local)
    keep = pltpu.make_async_copy(bank.at[pl.ds(first, local)], bank_hbm, sem.at[2 * group])
    keep.start()
    outs = [
        pltpu.make_async_copy(
            rel_v.at[j, pl.ds(h * half, half)], rel_hbm.at[j, pl.ds(h * half, half)], sem.at[2 * j + h]
        )
        for j in range(group)
        for h in range(2)
    ]
    for j in range(group):
        for h in range(2):
            part = slice(h * half, (h + 1) * half)
            r = lax.dot_general(q_v[j, part, :], bank[...], NT, preferred_element_type=jnp.float32)
            rel_v[j, part, :] = (r * scale).astype(jnp.bfloat16)
            outs[2 * j + h].start()
    for out in outs:
        out.wait()
    keep.wait()


def per_device(n, queries, new_keys, cache_keys, window_start, owner_slot):
    toks, group, dim = queries.shape
    ktoks, local = new_keys.shape[0], cache_keys.shape[0]
    blocks = window_start.shape[0]
    slots = n * local
    hbm_spec = pl.BlockSpec(memory_space=pltpu.HBM)
    vmem_spec = pl.BlockSpec(memory_space=pltpu.VMEM)
    bf16 = jnp.bfloat16
    short = n == len(HAND_UP) * 2 + 2
    sems = [pltpu.SemaphoreType.DMA((n,))] * 6
    if short:
        sems = (
            [pltpu.SemaphoreType.REGULAR((n,))]
            + [pltpu.SemaphoreType.DMA((n,))] * 2
            + [pltpu.SemaphoreType.DMA((n * n // 2,))]
            + [pltpu.SemaphoreType.DMA((n,))] * 6
        )
    q_held, bank = pl.pallas_call(
        functools.partial(line_kernel if short else refresh_kernel, n),
        out_shape=(
            pltpu.VMEM((group, toks, dim), bf16),
            pltpu.VMEM((slots, dim), bf16),
        ),
        in_specs=[hbm_spec] * 5,
        out_specs=(vmem_spec, vmem_spec),
        scratch_shapes=[
            pltpu.SMEM((blocks,), jnp.int32),
            pltpu.VMEM((1, blocks), jnp.int32),
            pltpu.VMEM((dim, group * toks), bf16),
            pltpu.VMEM((n, ktoks, dim), bf16),
            pltpu.VMEM((n, local, dim), bf16),
            pltpu.VMEM((blocks, dim), jnp.float32),
            pltpu.VMEM((n, blocks, dim), jnp.float32),
            pltpu.SemaphoreType.DMA((5,)),
        ] + sems,
        compiler_params=pltpu.CompilerParams(
            collective_id=0, has_side_effects=True, vmem_limit_bytes=VMEM - 2 * dim * (group * toks + slots) - 16384
        ),
        name="refresh",
    )(
        window_start,
        owner_slot.reshape(1, blocks),
        jnp.transpose(queries, (1, 0, 2)),
        new_keys.reshape(ktoks, dim),
        cache_keys.reshape(local, dim),
    )
    rel, own = pl.pallas_call(
        relate_kernel,
        out_shape=(
            jax.ShapeDtypeStruct((group, toks, slots), bf16),
            jax.ShapeDtypeStruct((local, dim), bf16),
        ),
        in_specs=[vmem_spec, vmem_spec],
        out_specs=(hbm_spec, hbm_spec),
        scratch_shapes=[
            pltpu.VMEM((group, toks, slots), bf16),
            pltpu.SemaphoreType.DMA((2 * group + 1,)),
        ],
        compiler_params=pltpu.CompilerParams(
            vmem_limit_bytes=2 * group * toks * slots + 16 * 1024 * 1024
        ),
        name="relate",
    )(q_held, bank)
    return jnp.transpose(rel, (1, 0, 2)), own[:, None, :]


def solution(mesh):
    spec = P("seq", "kvh", None)
    return jax.shard_map(
        functools.partial(per_device, mesh.shape["seq"]),
        mesh=mesh,
        in_specs=(spec, spec, spec, P(), P()),
        out_specs=(spec, spec),
        check_vma=False,
    )
```
